32 devices in a mesh: gx: 8 (over y, x, core), gy: 4 (over z).
Axes of the slice: x: 2, y: 2, z: 4, core: 2. Of those that a mesh axis runs over, the one named last changes fastest.
Arguments:
- flow_field: bfloat16 [4, 64, 1024, 512], P(None, None, ('gx', 'gy')), may hold values from -6 to 6
- cotangent: bfloat16 [4, 64, 1024, 512], P(None, None, ('gx', 'gy')), may hold values from -2 to 2
- spectral_weight: bfloat16 [128, 64, 64, 128], P(('gx', 'gy')), may hold values from -0.75 to 0.75
- local_weight: bfloat16 [64, 64], replicated, may hold values from -0.75 to 0.75
- channel_bias: float32 [64], replicated, may hold values from -3 to 3
Outputs:
- output_field: bfloat16 [4, 64, 1024, 512], P(None, None, ('gx', 'gy'))
- grad_field: bfloat16 [4, 64, 1024, 512], P(None, None, ('gx', 'gy'))
- grad_spectral: float32 [128, 64, 64, 128], P(('gx', 'gy'))
The draws below stay inside these ranges and needn't reach their ends.
All inputs are finite; a program needn't handle non-finite values.
Results may differ from the reference program's by a relative error of at most 0.014.
Values may be sent and summed in bfloat16 or wider, within the bound.
A program may use at most 128 MiB of HBM per device.

```python
import math
import jax
import jax.numpy as jnp
from jax import lax

C = 64
NX = 1024
NY = 512
MODES = 64
Z = 4
KC = 128


def level_of(stream_key, dims, cuts, low, high):
    level, own = 1.0, jax.random.fold_in(stream_key, 6)
    for axis_at, blocks in cuts:
        draws = jnp.exp(jax.random.uniform(jax.random.fold_in(own, axis_at), (blocks,), jnp.float32, low / len(cuts), high / len(cuts)))
        level = level * jnp.repeat(draws, dims[axis_at] // blocks).reshape([-1 if axis == axis_at else 1 for axis in range(len(dims))])
    return level


def centred(key, shape, width, bound, cuts=(), kind=jnp.bfloat16):
    factor_of = level_of(key, shape, cuts, -0.22, 0.18) if cuts else 1.0
    values = jax.random.normal(key, shape, jnp.float32) * width * factor_of
    return jnp.minimum(jnp.maximum(values, -bound), bound).astype(kind)


def setup_inputs(seed: int = 0) -> dict:
    splits = jax.random.split(jax.random.key(seed), 6)
    flow_field = centred(splits[0], (Z, C, NX, NY), 1.0, 6.0, ((2, 32),))
    cotangent = centred(splits[1], (Z, C, NX, NY), 0.3, 2.0, ((2, 32),))
    spectral_weight = centred(splits[2], (KC, C, C, KC), C ** -0.5, 0.75, ((0, 32),))
    local_weight = centred(splits[3], (C, C), C ** -0.5, 0.75)
    channel_bias = centred(splits[4], (C,), 0.5, 3.0, (), jnp.float32)
    return dict(flow_field=flow_field, cotangent=cotangent, spectral_weight=spectral_weight, local_weight=local_weight, channel_bias=channel_bias)


root_half = 0.7071067811865476
density_norm = 0.3989422804014327

def basis_table(positions, columns, cells, kept, factor):
    frequency = jnp.where(columns < kept, columns, columns - kept + 1)
    phases = positions[:, None] * frequency[None, :] % cells
    angles = phases.astype(jnp.float32) * (2.0 * math.pi / cells)
    values = jnp.where(columns[None, :] < kept, jnp.cos(angles), jnp.sin(angles))
    return (values * factor).astype(jnp.bfloat16)

def gelu_slope(values):
    cumulative = 0.5 * (1.0 + lax.erf(values * root_half))
    density = jnp.exp(-0.5 * values * values) * density_norm
    return cumulative + values * density

def reference(flow_field, cotangent, spectral_weight, local_weight, channel_bias):
    columns = jnp.arange(2 * MODES, dtype=jnp.int32)
    rows_x = jnp.arange(NX, dtype=jnp.int32)
    rows_y = jnp.arange(NY, dtype=jnp.int32)
    fwd_x = basis_table(rows_x, columns, NX, MODES, math.sqrt(2.0 / NX)).astype(jnp.float32)
    fwd_y = basis_table(rows_y, columns, NY, MODES, math.sqrt(2.0 / NY)).astype(jnp.float32)
    inv_x = basis_table(rows_x, columns, NX, MODES, math.sqrt(1.0 / MODES)).astype(jnp.float32)
    inv_y = basis_table(rows_y, columns, NY, MODES, math.sqrt(1.0 / MODES)).astype(jnp.float32)
    weights = spectral_weight.astype(jnp.float32)
    mixing = local_weight.astype(jnp.float32)

    def to_modes(plane, table_x, table_y):
        along = jnp.einsum('cxy,yj->cjx', plane.astype(jnp.float32), table_y).astype(jnp.bfloat16)
        return jnp.einsum('cjx,xk->cjk', along.astype(jnp.float32), table_x).astype(jnp.bfloat16)

    def to_space(modal, table_x, table_y):
        partial_x = jnp.einsum('cjk,xk->cjx', modal.astype(jnp.float32), table_x).astype(jnp.bfloat16)
        return jnp.einsum('cjx,yj->cxy', partial_x.astype(jnp.float32), table_y, precision=lax.Precision.HIGHEST)

    def plane_step(accum, inputs):
        plane, grad_out = inputs
        coeffs = to_modes(plane, fwd_x, fwd_y)
        mixed = jnp.einsum('ijk,jiok->ojk', coeffs.astype(jnp.float32), weights).astype(jnp.bfloat16)
        spectral = to_space(mixed, inv_x, inv_y)
        pointwise = jnp.einsum('ixy,io->oxy', plane.astype(jnp.float32), mixing)
        pre_activation = spectral + pointwise + channel_bias[:, None, None]
        output_plane = jax.nn.gelu(pre_activation, approximate=False).astype(jnp.bfloat16)
        grad_pre = (grad_out.astype(jnp.float32) * gelu_slope(pre_activation)).astype(jnp.bfloat16)
        grad_mixed = to_modes(grad_pre, inv_x, inv_y)
        accum = accum + jnp.einsum('ijk,ojk->jiok', coeffs.astype(jnp.float32), grad_mixed.astype(jnp.float32))
        grad_coeffs = jnp.einsum('ojk,jiok->ijk', grad_mixed.astype(jnp.float32), weights).astype(jnp.bfloat16)
        backward = to_space(grad_coeffs, fwd_x, fwd_y)
        grad_plane = (backward + jnp.einsum('oxy,io->ixy', grad_pre.astype(jnp.float32), mixing)).astype(jnp.bfloat16)
        return (accum, (output_plane, grad_plane))
    start = jnp.zeros((2 * MODES, C, C, 2 * MODES), jnp.float32)
    grad_spectral, (output_field, grad_field) = lax.scan(plane_step, start, (flow_field, cotangent))
    return (output_field, grad_field, grad_spectral)
```

```python
import functools
import math

import jax
import jax.numpy as jnp
import numpy as np
from jax import lax
from jax.experimental import pallas as pl
from jax.experimental.pallas import tpu as pltpu
from jax.sharding import PartitionSpec as P

root_half = 0.7071067811865476
density_norm = 0.3989422804014327
LANES = 128
PACK = 16
MESH = pl.DeviceIdType.MESH
f32, bf16 = jnp.float32, jnp.bfloat16


def basis_table(cells, cols, factor):
    kept = cols // 2
    columns = np.arange(cols)
    frequency = np.where(columns < kept, columns, columns - kept + 1)
    phases = np.arange(cells)[:, None] * frequency[None, :] % cells
    angles = phases.astype(np.float32) * np.float32(2.0 * math.pi / cells)
    values = np.where(columns[None, :] < kept, np.cos(angles), np.sin(angles))
    return jnp.asarray((values * np.float32(factor)).astype(jnp.bfloat16))


def gelu_slope(values):
    cumulative = 0.5 * (1.0 + lax.erf(values * root_half))
    density = jnp.exp(-0.5 * values * values) * density_norm
    return cumulative + values * density


def dot_t(a, b, da, db):
    return lax.dot_general(a, b, (((da,), (db,)), ((), ())), preferred_element_type=f32)


def to_owners(modal_rows):
    return lax.all_to_all(modal_rows, ("gx", "gy"), split_axis=0, concat_axis=1, tiled=True)


def to_slabs(modal_part):
    return lax.all_to_all(modal_part, ("gx", "gy"), split_axis=1, concat_axis=0, tiled=True)


def contract(spec, left, right):
    return jnp.einsum(spec, left, right, preferred_element_type=jnp.float32)


def plain_shards(flow_field, cotangent, spectral_weight, local_weight, channel_bias):
    devices = lax.axis_size("gx") * lax.axis_size("gy")
    planes, channels, slab_rows, cells_along = flow_field.shape
    cells_across = slab_rows * devices
    own_cols = spectral_weight.shape[0]
    mode_cols = spectral_weight.shape[3]
    kept_modes = mode_cols // 2
    both = planes * channels
    scale_inv = math.sqrt(1.0 / kept_modes)
    fwd_x = basis_table(cells_across, mode_cols, math.sqrt(2.0 / cells_across))
    fwd_y = basis_table(cells_along, mode_cols, math.sqrt(2.0 / cells_along))
    inv_x = basis_table(cells_across, mode_cols, scale_inv)
    inv_y = basis_table(cells_along, mode_cols, scale_inv)

    def to_modes(field, table_x, table_y):
        rows = contract("axy,yj->jxa", field.reshape(both, slab_rows, cells_along), table_y)
        received = to_owners(rows.astype(jnp.bfloat16))
        modes = contract("jxa,xk->jka", received, table_x).astype(jnp.bfloat16)
        return modes.reshape(own_cols, mode_cols, planes, channels)

    def to_rows(modes, table_x):
        merged = modes.reshape(own_cols, mode_cols, both)
        return to_slabs(contract("jka,xk->jxa", merged, table_x).astype(jnp.bfloat16))

    def to_space(rows, table_y):
        field = contract("jxa,yj->axy", rows, table_y)
        return field.reshape(planes, channels, slab_rows, cells_along)

    coeffs = to_modes(flow_field, fwd_x, fwd_y)
    mixed = contract("jkzi,jiok->jkzo", coeffs, spectral_weight).astype(jnp.bfloat16)
    gathered = to_rows(mixed, inv_x)
    spectral = to_space(gathered, inv_y)
    pointwise = contract("zixy,io->zoxy", flow_field, local_weight)
    pre_activation = spectral + pointwise + channel_bias[None, :, None, None]
    output_field = jax.nn.gelu(pre_activation, approximate=False).astype(jnp.bfloat16)
    grad_pre = (cotangent.astype(jnp.float32) * gelu_slope(pre_activation)).astype(jnp.bfloat16)
    grad_mixed = to_modes(grad_pre, inv_x, inv_y)
    grad_coeffs = contract("jkzo,jiok->jkzi", grad_mixed, spectral_weight).astype(jnp.bfloat16)
    gathered_back = to_rows(grad_coeffs, fwd_x)
    grad_spectral = contract("jkzi,jkzo->jiok", coeffs, grad_mixed)
    backward = to_space(gathered_back, fwd_y)
    through_local = contract("zoxy,io->zixy", grad_pre, local_weight)
    grad_field = (backward + through_local).astype(jnp.bfloat16)
    return (output_field, grad_field, grad_spectral)


def spectral_kernel(
    adjoint, nx, ny, planes, chans, slab, modes, own,
    field_hbm, yt_ref, ta_ref, ti_ref, w_hbm,
    g_hbm, coef_ref,
    fbuf, wbuf, tf, tinv, sbuf, rbuf, part, zs, zr, cf, gf, ms, zg, tg, lhs2, isb,
    load_sem, w_sem, own_sem, s1, r1, s2, r2, s3, r3, s4, r4,
):
    gx, gy = lax.axis_index("gx"), lax.axis_index("gy")
    per = LANES // slab
    groups = chans // per
    jg = modes // nx

    def load(p):
        return pltpu.make_async_copy(field_hbm.at[p], fbuf.at[p], load_sem.at[p])

    def load_w():
        return pltpu.make_async_copy(w_hbm, wbuf, w_sem)

    for p in range(planes):
        load(p).start()
    load_w().start()

    barrier = pltpu.get_barrier_semaphore()
    for o in range(1, nx):
        pl.semaphore_signal(barrier, inc=1, device_id=((gx + o) % nx, gy), device_id_type=MESH)
    for o in range(1, ny):
        pl.semaphore_signal(barrier, inc=1, device_id=(gx, (gy + o) % ny), device_id_type=MESH)

    tf[...] = jnp.zeros_like(tf)
    tinv[...] = jnp.zeros_like(tinv)
    for s in range(nx):
        for c in range(per):
            rows = pl.ds(s * LANES + c * slab, slab)
            cols = pl.ds(c * modes, modes)
            tf[rows, cols] = ta_ref[s, gy]
            tinv[rows, cols] = ti_ref[s, gy]

    def lane(g):
        return pl.ds(pl.multiple_of(g * LANES, LANES), LANES)

    def jrows(g):
        return pl.ds(pl.multiple_of(g * jg, jg), jg)

    def rows_out(p, o):
        to = (gx + o) % nx
        return pltpu.make_async_remote_copy(
            sbuf.at[p, to], rbuf.at[p, :, :, lane(gx)], s1.at[p, o], r1.at[p, o],
            device_id=(to, gy), device_id_type=MESH)

    def rows_in(p, o):
        src = (gx + nx - o) % nx
        return pltpu.make_async_remote_copy(
            sbuf.at[p, src], rbuf.at[p, :, :, lane(src)], s1.at[p, o], r1.at[p, o],
            device_id=(src, gy), device_id_type=MESH)

    def sums_out(p, o):
        to = (gy + o) % ny
        return pltpu.make_async_remote_copy(
            zs.at[p, to], zr.at[p, gy], s2.at[p, o], r2.at[p, o],
            device_id=(gx, to), device_id_type=MESH)

    def sums_in(p, o):
        src = (gy + ny - o) % ny
        return pltpu.make_async_remote_copy(
            zs.at[p, src], zr.at[p, src], s2.at[p, o], r2.at[p, o],
            device_id=(gx, src), device_id_type=MESH)

    def mixed_out(p, o):
        to = (gy + o) % ny
        return pltpu.make_async_remote_copy(
            ms.at[p], zg.at[p, gy], s3.at[p, o], r3.at[p, o],
            device_id=(gx, to), device_id_type=MESH)

    def mixed_in(p, o):
        src = (gy + ny - o) % ny
        return pltpu.make_async_remote_copy(
            ms.at[p], zg.at[p, src], s3.at[p, o], r3.at[p, o],
            device_id=(gx, src), device_id_type=MESH)

    def back_out(p, o):
        to = (gx + o) % nx
        return pltpu.make_async_remote_copy(
            isb.at[p, to], g_hbm.at[p, :, jrows(gx), :], s4.at[p, o], r4.at[p, o],
            device_id=(to, gy), device_id_type=MESH)

    def back_in(p, o):
        src = (gx + nx - o) % nx
        return pltpu.make_async_remote_copy(
            isb.at[p, src], g_hbm.at[p, :, jrows(src), :], s4.at[p, o], r4.at[p, o],
            device_id=(src, gy), device_id_type=MESH)

    def back_own(p):
        return pltpu.make_async_copy(isb.at[p, gx], g_hbm.at[p, :, jrows(gx), :], own_sem.at[p])

    def analyse(p):
        load(p).wait()

        def body(t, carry):
            x = fbuf[p, pl.ds(t * 2 * per, 2 * per)].reshape(2 * LANES, fbuf.shape[3])
            r = dot_t(yt_ref[...], x, 1, 1).astype(bf16)
            for h in range(2):
                sbuf[p, :, t * 2 + h] = r[:, h * LANES:(h + 1) * LANES].reshape(nx, jg, LANES)
            return carry

        lax.fori_loop(0, groups // 2, body, 0)
        rbuf[p, :, :, lane(gx)] = sbuf[p, gx]

    def across(p):
        for o in range(1, nx):
            rows_in(p, o).wait_recv()
        left = rbuf[p].reshape(groups * jg, nx * LANES)
        sums = jnp.dot(left, tf[...], preferred_element_type=f32)
        for g in range(groups):
            for c in range(per):
                part[pl.ds((g * per + c) * jg, jg), :] = sums[g * jg:(g + 1) * jg, c * modes:(c + 1) * modes]
        for j in range(jg):
            zs[p, j // own, j % own] = part[pl.ds(j, chans, stride=jg), :].astype(bf16)
        zr[p, gy] = zs[p, gy]
        for o in range(1, ny):
            sums_out(p, o).start()

    def mix(p):
        @pl.when(p == 0)
        def _():
            load_w().wait()

        for o in range(1, ny):
            sums_in(p, o).wait_recv()
        total = zr[p, 0].astype(f32)
        for s in range(1, ny):
            total = total + zr[p, s].astype(f32)
        coef = total.astype(bf16)
        coef_ref[p] = coef
        cf[...] = coef.astype(f32).reshape(own * chans, modes)
        for j in range(own):
            if adjoint:
                right = cf[pl.ds(j * chans, chans), :]

                def body(i, carry):
                    prod = wbuf[j, i].astype(f32) * right
                    gf[pl.ds(i, 1), :] = jnp.sum(prod, axis=0, keepdims=True)
                    return carry

                lax.fori_loop(0, chans, body, 0, unroll=8)
                ms[p, j] = gf[...].astype(bf16)
            else:

                def body(i, acc):
                    return acc + cf[pl.ds(j * chans + i, 1), :] * wbuf[j, i].astype(f32)

                acc = lax.fori_loop(0, chans, body, jnp.zeros((chans, modes), f32), unroll=8)
                ms[p, j] = acc.astype(bf16)
        zg[p, gy] = ms[p]
        for o in range(1, ny):
            mixed_out(p, o).start()

    def expand(p):
        for o in range(1, ny):
            mixed_in(p, o).wait_recv()
        tg[...] = zg[p].astype(f32).reshape(ny * own * chans, modes)
        for c in range(chans):
            lhs2[pl.ds((c // per) * jg, jg), pl.ds((c % per) * modes, modes)] = tg[pl.ds(c, jg, stride=chans), :].astype(bf16)

        def body(t, carry):
            rows = tinv[pl.ds(pl.multiple_of(t * 2 * LANES, LANES), 2 * LANES), :]
            r = dot_t(lhs2[...], rows, 1, 1).astype(bf16)
            for h in range(2):
                isb[p, t * 2 + h] = r[:, h * LANES:(h + 1) * LANES].reshape(groups, jg, LANES)
            return carry

        lax.fori_loop(0, nx // 2, body, 0)
        back_own(p).start()
        for o in range(1, nx):
            back_out(p, o).start()

    analyse(0)
    pl.semaphore_wait(barrier, nx + ny - 2)
    for o in range(1, nx):
        rows_out(0, o).start()

    def first(p, carry):
        analyse(p)
        for o in range(1, nx):
            rows_out(p, o).start()
        return carry

    lax.fori_loop(1, planes, first, 0)

    def step(t, carry):
        @pl.when(t < planes)
        def _():
            across(t)

        @pl.when((t >= 1) & (t <= planes))
        def _():
            mix(t - 1)

        @pl.when(t >= 2)
        def _():
            expand(t - 2)

        return carry

    lax.fori_loop(0, planes + 2, step, 0)

    def finish(p, carry):
        for o in range(1, nx):
            rows_out(p, o).wait_send()
            back_out(p, o).wait_send()
            back_in(p, o).wait_recv()
        for o in range(1, ny):
            sums_out(p, o).wait_send()
            mixed_out(p, o).wait_send()
        back_own(p).wait()
        return carry

    lax.fori_loop(0, planes, finish, 0)


def spectral_pass(adjoint, nx, ny, field, table_y, table_a, table_i, weight):
    planes, chans, slab, cells = field.shape
    own, modes = weight.shape[0], weight.shape[3]
    per = LANES // slab
    groups = chans // per
    jg = modes // nx
    vm = pl.BlockSpec(memory_space=pltpu.VMEM)
    hbm = pl.BlockSpec(memory_space=pl.ANY)
    dma = pltpu.SemaphoreType.DMA
    split = lambda t: t.reshape(nx, ny, slab, modes)
    return pl.pallas_call(
        functools.partial(spectral_kernel, adjoint, nx, ny, planes, chans, slab, modes, own),
        out_shape=(
            jax.ShapeDtypeStruct((planes, groups, modes, LANES), bf16),
            jax.ShapeDtypeStruct((planes, own, chans, modes), bf16),
        ),
        in_specs=[hbm, vm, vm, vm, hbm],
        out_specs=(hbm, vm),
        scratch_shapes=[
            pltpu.VMEM((planes, chans, slab, cells), bf16),
            pltpu.VMEM((own, chans, chans, modes), bf16),
            pltpu.VMEM((nx * LANES, per * modes), bf16),
            pltpu.VMEM((nx * LANES, per * modes), bf16),
            pltpu.VMEM((planes, nx, groups, jg, LANES), bf16),
            pltpu.VMEM((planes, groups, jg, nx * LANES), bf16),
            pltpu.VMEM((chans * jg, modes), f32),
            pltpu.VMEM((planes, ny, own, chans, modes), bf16),
            pltpu.VMEM((planes, ny, own, chans, modes), bf16),
            pltpu.VMEM((own * chans, modes), f32),
            pltpu.VMEM((chans, modes), f32),
            pltpu.VMEM((planes, own, chans, modes), bf16),
            pltpu.VMEM((planes, ny, own, chans, modes), bf16),
            pltpu.VMEM((ny * own * chans, modes), f32),
            pltpu.VMEM((groups * jg, per * modes), bf16),
            pltpu.VMEM((planes, nx, groups, jg, LANES), bf16),
            dma((planes,)), dma, dma((planes,)),
            dma((planes, nx)), dma((planes, nx)),
            dma((planes, ny)), dma((planes, ny)),
            dma((planes, ny)), dma((planes, ny)),
            dma((planes, nx)), dma((planes, nx)),
        ],
        compiler_params=pltpu.CompilerParams(
            collective_id=1 if adjoint else 0, has_side_effects=True,
            vmem_limit_bytes=48 << 20),
        name="spectral_back" if adjoint else "spectral_fwd",
    )(field, table_y.T, split(table_a), split(table_i), weight)


def forward_kernel(flow_ref, cot_ref, g_ref, yt_ref, kr_ref, bias_ref, out_ref, gp_ref, pre, xs):
    _, chans, slab, width = flow_ref.shape
    groups = g_ref.shape[1]
    per = chans // groups

    def modal(g, carry):
        r = dot_t(g_ref[0, g], yt_ref[...], 0, 0)
        pre[pl.ds(g * per, per)] = r.reshape(per, slab, width)
        return carry

    lax.fori_loop(0, groups, modal, 0)
    for h in range(slab // PACK):
        xs[...] = flow_ref[0, :, h * PACK:(h + 1) * PACK, :].reshape(chans * PACK, width)

        def local(t, carry):
            r = jnp.dot(kr_ref[pl.ds(t * PACK * PACK, PACK * PACK), :], xs[...], preferred_element_type=f32)
            rows = pl.ds(t * PACK, PACK)
            pre[rows, h * PACK:(h + 1) * PACK, :] += r.reshape(PACK, PACK, width)
            return carry

        lax.fori_loop(0, chans // PACK, local, 0)

    def point(c, carry):
        v = pre[c] + bias_ref[c]
        phi = 0.5 + 0.5 * lax.erf(v * root_half)
        density = jnp.exp(-0.5 * v * v) * density_norm
        out_ref[0, c] = (v * phi).astype(bf16)
        gp_ref[0, c] = (cot_ref[0, c].astype(f32) * (phi + v * density)).astype(bf16)
        return carry

    lax.fori_loop(0, chans, point, 0, unroll=2)


def forward_space(flow, cot, g, table_y, kron, bias, parts):
    planes, chans, slab, cells = flow.shape
    groups, modes = g.shape[1], g.shape[2]
    width = cells // parts
    field = pl.BlockSpec((1, chans, slab, width), lambda p, h: (p, 0, 0, h))
    shape = jax.ShapeDtypeStruct(flow.shape, bf16)
    return pl.pallas_call(
        forward_kernel,
        grid=(planes, parts),
        out_shape=(shape, shape),
        in_specs=[
            field, field,
            pl.BlockSpec((1, groups, modes, LANES), lambda p, h: (p, 0, 0, 0)),
            pl.BlockSpec((modes, width), lambda p, h: (0, h)),
            pl.BlockSpec(kron.shape, lambda p, h: (0, 0), pipeline_mode=pl.Buffered(1)),
            pl.BlockSpec(memory_space=pltpu.SMEM),
        ],
        out_specs=(field, field),
        scratch_shapes=[
            pltpu.VMEM((chans, slab, width), f32),
            pltpu.VMEM((chans * PACK, width), bf16),
        ],
        compiler_params=pltpu.CompilerParams(vmem_limit_bytes=56 << 20),
        name="forward_space",
    )(flow, cot, g, table_y.T, kron, bias)


def backward_kernel(gp_ref, g_ref, yt_ref, kr_ref, co_ref, gm_ref, out_ref, gs_ref, acc, xs, cf):
    _, chans, slab, width = gp_ref.shape
    groups = g_ref.shape[1]
    per = chans // groups
    planes, rows_here = co_ref.shape[0], co_ref.shape[1]

    def modal(g, carry):
        r = dot_t(g_ref[0, g], yt_ref[...], 0, 0)
        acc[pl.ds(g * per, per)] = r.reshape(per, slab, width)
        return carry

    lax.fori_loop(0, groups, modal, 0)
    for h in range(slab // PACK):
        xs[...] = gp_ref[0, :, h * PACK:(h + 1) * PACK, :].reshape(chans * PACK, width)

        def local(t, carry):
            r = jnp.dot(kr_ref[pl.ds(t * PACK * PACK, PACK * PACK), :], xs[...], preferred_element_type=f32)
            rows = pl.ds(t * PACK, PACK)
            base = acc[rows, h * PACK:(h + 1) * PACK, :]
            out_ref[0, rows, h * PACK:(h + 1) * PACK, :] = (base + r.reshape(PACK, PACK, width)).astype(bf16)
            return carry

        lax.fori_loop(0, chans // PACK, local, 0)

    cf[...] = co_ref[...].astype(f32).reshape(cf.shape)

    def outer(r, carry):
        total = cf[pl.ds(r, 1), :] * gm_ref[0, 0].astype(f32)
        for p in range(1, planes):
            total = total + cf[pl.ds(p * rows_here + r, 1), :] * gm_ref[p, 0].astype(f32)
        gs_ref[r] = total
        return carry

    lax.fori_loop(0, rows_here, outer, 0, unroll=4)


def backward_space(gp, g, table_y, kron, co, gm, parts):
    planes, chans, slab, cells = gp.shape
    groups, modes = g.shape[1], g.shape[2]
    own = co.shape[1]
    width = cells // parts
    rows_here = own * chans // (planes * parts)
    field = pl.BlockSpec((1, chans, slab, width), lambda p, h: (p, 0, 0, h))
    return pl.pallas_call(
        backward_kernel,
        grid=(planes, parts),
        out_shape=(
            jax.ShapeDtypeStruct(gp.shape, bf16),
            jax.ShapeDtypeStruct((own * chans, chans, modes), f32),
        ),
        in_specs=[
            field,
            pl.BlockSpec((1, groups, modes, LANES), lambda p, h: (p, 0, 0, 0)),
            pl.BlockSpec((modes, width), lambda p, h: (0, h)),
            pl.BlockSpec(kron.shape, lambda p, h: (0, 0), pipeline_mode=pl.Buffered(1)),
            pl.BlockSpec((planes, rows_here, modes), lambda p, h: (0, p * parts + h, 0)),
            pl.BlockSpec((planes, 1, chans, modes), lambda p, h: (0, (p * parts + h) * rows_here // chans, 0, 0)),
        ],
        out_specs=(field, pl.BlockSpec((rows_here, chans, modes), lambda p, h: (p * parts + h, 0, 0))),
        scratch_shapes=[
            pltpu.VMEM((chans, slab, width), f32),
            pltpu.VMEM((chans * PACK, width), bf16),
            pltpu.VMEM((planes * rows_here, modes), f32),
        ],
        compiler_params=pltpu.CompilerParams(vmem_limit_bytes=56 << 20),
        name="backward_space",
    )(gp, g, table_y.T, kron, co.reshape(planes, own * chans, modes), gm)


def spread(matrix):
    rows = matrix.shape[0] * PACK
    index = jnp.arange(rows)
    pick = (index[:, None] // PACK == jnp.arange(matrix.shape[0])[None, :]).astype(bf16)
    full = jnp.dot(jnp.dot(pick, matrix, preferred_element_type=bf16), pick.T, preferred_element_type=bf16)
    return jnp.where(index[:, None] % PACK == index[None, :] % PACK, full, jnp.zeros_like(full))


def kernel_shards(nx, ny, flow_field, cotangent, spectral_weight, local_weight, channel_bias):
    planes, chans, slab, cells = flow_field.shape
    across = slab * nx * ny
    own, modes = spectral_weight.shape[0], spectral_weight.shape[3]
    scale_inv = math.sqrt(1.0 / (modes // 2))
    fwd_x = basis_table(across, modes, math.sqrt(2.0 / across))
    fwd_y = basis_table(cells, modes, math.sqrt(2.0 / cells))
    inv_x = basis_table(across, modes, scale_inv)
    inv_y = basis_table(cells, modes, scale_inv)
    parts = 2
    g, coeffs = spectral_pass(False, nx, ny, flow_field, fwd_y, fwd_x, inv_x, spectral_weight)
    out, grad_pre = forward_space(flow_field, cotangent, g, inv_y, spread(local_weight.T), channel_bias, parts)
    back, grad_mixed = spectral_pass(True, nx, ny, grad_pre, inv_y, inv_x, fwd_x, spectral_weight)
    grad_field, grad_spectral = backward_space(grad_pre, back, fwd_y, spread(local_weight), coeffs, grad_mixed, parts)
    return out, grad_field, grad_spectral.reshape(own, chans, chans, modes)


def solution(mesh):
    nx, ny = mesh.shape["gx"], mesh.shape["gy"]

    def shards(flow_field, cotangent, spectral_weight, local_weight, channel_bias):
        planes, chans, slab, cells = flow_field.shape
        own, modes = spectral_weight.shape[0], spectral_weight.shape[3]
        fits = (
            slab % PACK == 0 and LANES % slab == 0 and modes == LANES
            and nx % 2 == 0 and (modes // nx) % PACK == 0
            and chans % (2 * LANES // slab) == 0 and chans % PACK == 0
            and cells % (2 * LANES) == 0
            and own * nx * ny == modes and chans % (own * chans // (2 * planes)) == 0
        )
        args = (flow_field, cotangent, spectral_weight, local_weight, channel_bias)
        return kernel_shards(nx, ny, *args) if fits else plain_shards(*args)

    placed = (
        P(None, None, ("gx", "gy"), None),
        P(None, None, ("gx", "gy"), None),
        P(("gx", "gy"), None, None, None),
        P(),
        P(),
    )
    return jax.shard_map(
        shards,
        mesh=mesh,
        in_specs=placed,
        out_specs=(
            P(None, None, ("gx", "gy"), None),
            P(None, None, ("gx", "gy"), None),
            P(("gx", "gy"), None, None, None),
        ),
        check_vma=False,
    )
```

```python
import functools
import math

import jax
import jax.numpy as jnp
import numpy as np
from jax import lax
from jax.experimental import pallas as pl
from jax.experimental.pallas import tpu as pltpu
from jax.sharding import PartitionSpec as P

root_half = 0.7071067811865476
density_norm = 0.3989422804014327
LANES = 128
PACK = 16
MESH = pl.DeviceIdType.MESH
f32, bf16 = jnp.float32, jnp.bfloat16


def basis_table(cells, cols, factor):
    kept = cols // 2
    columns = np.arange(cols)
    frequency = np.where(columns < kept, columns, columns - kept + 1)
    phases = np.arange(cells)[:, None] * frequency[None, :] % cells
    angles = phases.astype(np.float32) * np.float32(2.0 * math.pi / cells)
    values = np.where(columns[None, :] < kept, np.cos(angles), np.sin(angles))
    return jnp.asarray((values * np.float32(factor)).astype(jnp.bfloat16))


def gelu_slope(values):
    cumulative = 0.5 * (1.0 + lax.erf(values * root_half))
    density = jnp.exp(-0.5 * values * values) * density_norm
    return cumulative + values * density


def dot_t(a, b, da, db):
    return lax.dot_general(a, b, (((da,), (db,)), ((), ())), preferred_element_type=f32)


def to_owners(modal_rows):
    return lax.all_to_all(modal_rows, ("gx", "gy"), split_axis=0, concat_axis=1, tiled=True)


def to_slabs(modal_part):
    return lax.all_to_all(modal_part, ("gx", "gy"), split_axis=1, concat_axis=0, tiled=True)


def contract(spec, left, right):
    return jnp.einsum(spec, left, right, preferred_element_type=jnp.float32)


def plain_shards(flow_field, cotangent, spectral_weight, local_weight, channel_bias):
    devices = lax.axis_size("gx") * lax.axis_size("gy")
    planes, channels, slab_rows, cells_along = flow_field.shape
    cells_across = slab_rows * devices
    own_cols = spectral_weight.shape[0]
    mode_cols = spectral_weight.shape[3]
    kept_modes = mode_cols // 2
    both = planes * channels
    scale_inv = math.sqrt(1.0 / kept_modes)
    fwd_x = basis_table(cells_across, mode_cols, math.sqrt(2.0 / cells_across))
    fwd_y = basis_table(cells_along, mode_cols, math.sqrt(2.0 / cells_along))
    inv_x = basis_table(cells_across, mode_cols, scale_inv)
    inv_y = basis_table(cells_along, mode_cols, scale_inv)

    def to_modes(field, table_x, table_y):
        rows = contract("axy,yj->jxa", field.reshape(both, slab_rows, cells_along), table_y)
        received = to_owners(rows.astype(jnp.bfloat16))
        modes = contract("jxa,xk->jka", received, table_x).astype(jnp.bfloat16)
        return modes.reshape(own_cols, mode_cols, planes, channels)

    def to_rows(modes, table_x):
        merged = modes.reshape(own_cols, mode_cols, both)
        return to_slabs(contract("jka,xk->jxa", merged, table_x).astype(jnp.bfloat16))

    def to_space(rows, table_y):
        field = contract("jxa,yj->axy", rows, table_y)
        return field.reshape(planes, channels, slab_rows, cells_along)

    coeffs = to_modes(flow_field, fwd_x, fwd_y)
    mixed = contract("jkzi,jiok->jkzo", coeffs, spectral_weight).astype(jnp.bfloat16)
    gathered = to_rows(mixed, inv_x)
    spectral = to_space(gathered, inv_y)
    pointwise = contract("zixy,io->zoxy", flow_field, local_weight)
    pre_activation = spectral + pointwise + channel_bias[None, :, None, None]
    output_field = jax.nn.gelu(pre_activation, approximate=False).astype(jnp.bfloat16)
    grad_pre = (cotangent.astype(jnp.float32) * gelu_slope(pre_activation)).astype(jnp.bfloat16)
    grad_mixed = to_modes(grad_pre, inv_x, inv_y)
    grad_coeffs = contract("jkzo,jiok->jkzi", grad_mixed, spectral_weight).astype(jnp.bfloat16)
    gathered_back = to_rows(grad_coeffs, fwd_x)
    grad_spectral = contract("jkzi,jkzo->jiok", coeffs, grad_mixed)
    backward = to_space(gathered_back, fwd_y)
    through_local = contract("zoxy,io->zixy", grad_pre, local_weight)
    grad_field = (backward + through_local).astype(jnp.bfloat16)
    return (output_field, grad_field, grad_spectral)


def main_kernel(
    nx, ny, planes, chans, slab, modes, own,
    flow_hbm, cot_hbm, w_hbm, lw_ref, bias_ref, fy_ref, iy_ref, fx_ref, ix_ref,
    out_hbm, gp_hbm, back_hbm, kron_hbm, co_ref, gm_ref,
    fbuf, cbuf, wbuf, tx, kron, kron_t, sbuf, rbuf, part, zs, zr, cf, gf, ms, zg, tg, lhs2, isb,
    gbuf, gt, pre, xs,
    load_sem, cot_sem, store_sem, w_sem, kron_sem, own_sem, s1, r1, s2, r2, s3, r3, s4, r4,
):
    gx, gy = lax.axis_index("gx"), lax.axis_index("gy")
    per = LANES // slab
    groups = chans // per
    jg = modes // nx
    cells = fbuf.shape[3]
    halves = slab // PACK
    width = 2 * LANES
    parts = cells // width

    def load(p):
        return pltpu.make_async_copy(flow_hbm.at[p], fbuf.at[p], load_sem.at[p])

    def load_cot(p):
        return pltpu.make_async_copy(cot_hbm.at[p], cbuf.at[p], cot_sem.at[p])

    def store_out(p):
        return pltpu.make_async_copy(cbuf.at[p], out_hbm.at[p], store_sem.at[0, p])

    def store_gp(p):
        return pltpu.make_async_copy(fbuf.at[p], gp_hbm.at[p], store_sem.at[1, p])

    def load_w():
        return pltpu.make_async_copy(w_hbm, wbuf, w_sem)

    def store_kron():
        return pltpu.make_async_copy(kron_t, kron_hbm, kron_sem)

    for p in range(planes):
        load(p).start()
    load_w().start()
    for p in range(planes):
        load_cot(p).start()

    barrier = pltpu.get_barrier_semaphore()
    for o in range(1, nx):
        pl.semaphore_signal(barrier, inc=1, device_id=((gx + o) % nx, gy), device_id_type=MESH)
    for o in range(1, ny):
        pl.semaphore_signal(barrier, inc=1, device_id=(gx, (gy + o) % ny), device_id_type=MESH)

    def lane(g):
        return pl.ds(pl.multiple_of(g * LANES, LANES), LANES)

    def jrows(g):
        return pl.ds(pl.multiple_of(g * jg, jg), jg)

    def rows(f, p, o, out):
        other = (gx + o) % nx if out else (gx + nx - o) % nx
        slot = gx if out else other
        return pltpu.make_async_remote_copy(
            sbuf.at[f, p, other], rbuf.at[f, p, :, :, lane(slot)], s1.at[f, p, o], r1.at[f, p, o],
            device_id=(other, gy), device_id_type=MESH)

    def sums(f, p, o, out):
        other = (gy + o) % ny if out else (gy + ny - o) % ny
        slot = gy if out else other
        return pltpu.make_async_remote_copy(
            zs.at[f, p, other], zr.at[f, p, slot], s2.at[f, p, o], r2.at[f, p, o],
            device_id=(gx, other), device_id_type=MESH)

    def mixed(f, p, o, out):
        other = (gy + o) % ny if out else (gy + ny - o) % ny
        slot = gy if out else other
        return pltpu.make_async_remote_copy(
            ms.at[f, p], zg.at[f, p, slot], s3.at[f, p, o], r3.at[f, p, o],
            device_id=(gx, other), device_id_type=MESH)

    def back(f, p, o, out):
        other = (gx + o) % nx if out else (gx + nx - o) % nx
        slot = gx if out else other
        into = back_hbm if f else gbuf
        return pltpu.make_async_remote_copy(
            isb.at[f, p, other], into.at[p, :, jrows(slot), :], s4.at[f, p, o], r4.at[f, p, o],
            device_id=(other, gy), device_id_type=MESH)

    def back_own(p):
        return pltpu.make_async_copy(isb.at[1, p, gx], back_hbm.at[p, :, jrows(gx), :], own_sem.at[p])

    def analyse(f, p):
        table = iy_ref if f else fy_ref

        def body(t, carry):
            x = fbuf[p, pl.ds(t * 2 * per, 2 * per)].reshape(2 * LANES, cells)
            r = dot_t(table[...], x, 1, 1).astype(bf16)
            for h in range(2):
                sbuf[f, p, :, t * 2 + h] = r[:, h * LANES:(h + 1) * LANES].reshape(nx, jg, LANES)
            return carry

        lax.fori_loop(0, groups // 2, body, 0, unroll=2)
        rbuf[f, p, :, :, lane(gx)] = sbuf[f, p, gx]

    def send_rows(f, p):
        for o in range(1, nx):
            rows(f, p, o, True).start()

    def across(f, p):
        for o in range(1, nx):
            rows(f, p, o, False).wait_recv()
        left = rbuf[f, p].reshape(groups * jg, nx * LANES)
        r = jnp.dot(left, tx[f], preferred_element_type=f32)
        for g in range(groups):
            for c in range(per):
                part[pl.ds((g * per + c) * jg, jg), :] = r[g * jg:(g + 1) * jg, c * modes:(c + 1) * modes]
        for j in range(jg):
            zs[f, p, j // own, j % own] = part[pl.ds(j, chans, stride=jg), :].astype(bf16)
        zr[f, p, gy] = zs[f, p, gy]
        for o in range(1, ny):
            sums(f, p, o, True).start()

    def mix(f, p):
        for o in range(1, ny):
            sums(f, p, o, False).wait_recv()
        total = zr[f, p, 0].astype(f32)
        for s in range(1, ny):
            total = total + zr[f, p, s].astype(f32)
        coef = total.astype(bf16)
        if f:
            gm_ref[p] = coef
        else:
            co_ref[p] = coef
        cf[...] = coef.astype(f32).reshape(own * chans, modes)
        for j in range(own):
            if f:
                right = cf[pl.ds(j * chans, chans), :]

                def body(i, carry):
                    prod = wbuf[j, i].astype(f32) * right
                    gf[pl.ds(i, 1), :] = jnp.sum(prod, axis=0, keepdims=True)
                    return carry

                lax.fori_loop(0, chans, body, 0, unroll=8)
                ms[f, p, j] = gf[...].astype(bf16)
            else:

                def body(i, acc):
                    return acc + cf[pl.ds(j * chans + i, 1), :] * wbuf[j, i].astype(f32)

                acc = lax.fori_loop(0, chans, body, jnp.zeros((chans, modes), f32), unroll=8)
                ms[f, p, j] = acc.astype(bf16)
        zg[f, p, gy] = ms[f, p]
        for o in range(1, ny):
            mixed(f, p, o, True).start()

    def expand(f, p):
        for o in range(1, ny):
            mixed(f, p, o, False).wait_recv()
        tg[...] = zg[f, p].astype(f32).reshape(ny * own * chans, modes)
        for c in range(chans):
            lhs2[pl.ds((c // per) * jg, jg), pl.ds((c % per) * modes, modes)] = tg[pl.ds(c, jg, stride=chans), :].astype(bf16)

        def body(t, carry):
            table = tx[1 - f, pl.ds(pl.multiple_of(t * 2 * LANES, LANES), 2 * LANES), :]
            r = dot_t(lhs2[...], table, 1, 1).astype(bf16)
            for h in range(2):
                isb[f, p, t * 2 + h] = r[:, h * LANES:(h + 1) * LANES].reshape(groups, jg, LANES)
            return carry

        lax.fori_loop(0, nx // 2, body, 0, unroll=2)
        if f:
            back_own(p).start()
        else:
            gbuf[p, :, jrows(gx), :] = isb[f, p, gx]
        for o in range(1, nx):
            back(f, p, o, True).start()

    def point(p):
        load_cot(p).wait()
        for o in range(1, nx):
            back(0, p, o, False).wait_recv()

        def turn(g, carry):
            block = gbuf[p, g].T.reshape(per, halves, PACK, modes)
            for h in range(halves):
                gt[h, pl.ds(g * per * PACK, per * PACK), :] = block[:, h].reshape(per * PACK, modes)
            return carry

        lax.fori_loop(0, groups, turn, 0, unroll=4)

        def piece(s, carry):
            h, y = s // parts, s % parts
            rows16 = pl.ds(pl.multiple_of(h * PACK, PACK), PACK)
            cols = pl.ds(pl.multiple_of(y * width, width), width)
            xs[...] = fbuf[p, :, rows16, cols].reshape(chans * PACK, width)
            r = jnp.dot(kron[...], xs[...], preferred_element_type=f32)
            r = r + jnp.dot(gt[h], iy_ref[:, cols], preferred_element_type=f32)
            pre[...] = r.reshape(chans, PACK, width)

            def one(c, inner):
                v = pre[c] + bias_ref[c]
                phi = 0.5 + 0.5 * lax.erf(v * root_half)
                density = jnp.exp(-0.5 * v * v) * density_norm
                cot = cbuf[p, c, rows16, cols].astype(f32)
                cbuf[p, c, rows16, cols] = (v * phi).astype(bf16)
                fbuf[p, c, rows16, cols] = (cot * (phi + v * density)).astype(bf16)
                return inner

            lax.fori_loop(0, chans, one, 0, unroll=4)
            return carry

        lax.fori_loop(0, halves * parts, piece, 0)
        store_out(p).start()
        store_gp(p).start()

    load(0).wait()
    analyse(0, 0)
    pl.semaphore_wait(barrier, nx + ny - 2)
    send_rows(0, 0)

    def first(p, carry):
        load(p).wait()
        analyse(0, p)
        send_rows(0, p)
        return carry

    lax.fori_loop(1, planes, first, 0)

    tx[...] = jnp.zeros_like(tx)
    for f, ref in enumerate((fx_ref, ix_ref)):
        for s in range(nx):
            for c in range(per):
                tx[f, pl.ds(s * LANES + c * slab, slab), pl.ds(c * modes, modes)] = ref[s, gy]

    tall = chans * PACK
    row = lax.broadcasted_iota(jnp.int32, (tall, chans), 0) // PACK
    col = lax.broadcasted_iota(jnp.int32, (tall, chans), 1)
    pick = jnp.where(row == col, 1.0, 0.0).astype(bf16)
    right = dot_t(lw_ref[...], pick, 1, 1).astype(bf16)
    left = dot_t(lw_ref[...], pick, 0, 1).astype(bf16)
    cut = 2 * LANES
    for k in range(tall // cut):
        sub = pick[k * cut:(k + 1) * cut]
        keep = (lax.broadcasted_iota(jnp.int32, (cut, tall), 0) % PACK
                == lax.broadcasted_iota(jnp.int32, (cut, tall), 1) % PACK)
        rows_k = pl.ds(k * cut, cut)
        kron_t[rows_k, :] = jnp.where(keep, jnp.dot(sub, right, preferred_element_type=f32), 0.0).astype(bf16)
        kron[rows_k, :] = jnp.where(keep, jnp.dot(sub, left, preferred_element_type=f32), 0.0).astype(bf16)
    store_kron().start()
    load_w().wait()

    def step(t, carry):
        def stage(lag, run):
            @pl.when((t >= lag) & (t < planes + lag))
            def _():
                run(t - lag)

        def middle(p):
            point(p)
            analyse(1, p)
            send_rows(1, p)

        stage(0, functools.partial(across, 0))
        stage(1, functools.partial(mix, 0))
        stage(2, functools.partial(expand, 0))
        stage(3, middle)
        stage(4, functools.partial(across, 1))
        stage(5, functools.partial(mix, 1))
        stage(6, functools.partial(expand, 1))
        return carry

    lax.fori_loop(0, planes + 6, step, 0)

    def finish(p, carry):
        for f in range(2):
            for o in range(1, nx):
                rows(f, p, o, True).wait_send()
                back(f, p, o, True).wait_send()
            for o in range(1, ny):
                sums(f, p, o, True).wait_send()
                mixed(f, p, o, True).wait_send()
        for o in range(1, nx):
            back(1, p, o, False).wait_recv()
        back_own(p).wait()
        store_out(p).wait()
        store_gp(p).wait()
        return carry

    lax.fori_loop(0, planes, finish, 0)
    store_kron().wait()


def main_pass(nx, ny, flow, cot, weight, local_weight, bias, fwd_y, inv_y, fwd_x, inv_x):
    planes, chans, slab, cells = flow.shape
    own, modes = weight.shape[0], weight.shape[3]
    per = LANES // slab
    groups = chans // per
    jg = modes // nx
    tall = chans * PACK
    vm = pl.BlockSpec(memory_space=pltpu.VMEM)
    hbm = pl.BlockSpec(memory_space=pl.ANY)
    dma = pltpu.SemaphoreType.DMA
    split = lambda t: t.reshape(nx, ny, slab, modes)
    field = jax.ShapeDtypeStruct(flow.shape, bf16)
    coef = jax.ShapeDtypeStruct((planes, own, chans, modes), bf16)
    return pl.pallas_call(
        functools.partial(main_kernel, nx, ny, planes, chans, slab, modes, own),
        out_shape=(
            field, field,
            jax.ShapeDtypeStruct((planes, groups, modes, LANES), bf16),
            jax.ShapeDtypeStruct((tall, tall), bf16),
            coef, coef,
        ),
        in_specs=[hbm, hbm, hbm, vm, pl.BlockSpec(memory_space=pltpu.SMEM), vm, vm, vm, vm],
        out_specs=(hbm, hbm, hbm, hbm, vm, vm),
        scratch_shapes=[
            pltpu.VMEM(flow.shape, bf16),
            pltpu.VMEM(flow.shape, bf16),
            pltpu.VMEM(weight.shape, bf16),
            pltpu.VMEM((2, nx * LANES, per * modes), bf16),
            pltpu.VMEM((tall, tall), bf16),
            pltpu.VMEM((tall, tall), bf16),
            pltpu.VMEM((2, planes, nx, groups, jg, LANES), bf16),
            pltpu.VMEM((2, planes, groups, jg, nx * LANES), bf16),
            pltpu.VMEM((chans * jg, modes), f32),
            pltpu.VMEM((2, planes, ny, own, chans, modes), bf16),
            pltpu.VMEM((2, planes, ny, own, chans, modes), bf16),
            pltpu.VMEM((own * chans, modes), f32),
            pltpu.VMEM((chans, modes), f32),
            pltpu.VMEM((2, planes, own, chans, modes), bf16),
            pltpu.VMEM((2, planes, ny, own, chans, modes), bf16),
            pltpu.VMEM((ny * own * chans, modes), f32),
            pltpu.VMEM((groups * jg, per * modes), bf16),
            pltpu.VMEM((2, planes, nx, groups, jg, LANES), bf16),
            pltpu.VMEM((planes, groups, modes, LANES), bf16),
            pltpu.VMEM((slab // PACK, tall, modes), bf16),
            pltpu.VMEM((chans, PACK, 2 * LANES), f32),
            pltpu.VMEM((tall, 2 * LANES), bf16),
            dma((planes,)), dma((planes,)), dma((2, planes)), dma, dma, dma((planes,)),
            dma((2, planes, nx)), dma((2, planes, nx)),
            dma((2, planes, ny)), dma((2, planes, ny)),
            dma((2, planes, ny)), dma((2, planes, ny)),
            dma((2, planes, nx)), dma((2, planes, nx)),
        ],
        compiler_params=pltpu.CompilerParams(
            collective_id=0, has_side_effects=True, vmem_limit_bytes=62 << 20),
        name="main_pass",
    )(flow, cot, weight, local_weight, bias, fwd_y.T, inv_y.T, split(fwd_x), split(inv_x))


def rows_by_half(g_ref, gt):
    groups = g_ref.shape[1]
    halves, tall, modes = gt.shape
    slab = halves * PACK
    per = LANES // slab

    def turn(g, carry):
        block = g_ref[0, g].T.reshape(per, halves, PACK, modes)
        for h in range(halves):
            gt[h, pl.ds(g * per * PACK, per * PACK), :] = block[:, h].reshape(per * PACK, modes)
        return carry

    lax.fori_loop(0, groups, turn, 0, unroll=4)


def backward_kernel(gp_ref, g_ref, yt_ref, kr_ref, co_ref, gm_ref, held_ref, out_ref, gs_ref, keep_ref, xs, gt, cf):
    _, chans, slab, width = gp_ref.shape
    planes, rows_here = co_ref.shape[0], co_ref.shape[1]

    @pl.when(pl.program_id(1) == 0)
    def _():
        rows_by_half(g_ref, gt)

    for h in range(slab // PACK):
        xs[...] = gp_ref[0, :, h * PACK:(h + 1) * PACK, :].reshape(chans * PACK, width)
        r = jnp.dot(kr_ref[...], xs[...], preferred_element_type=f32)
        r = r + jnp.dot(gt[h], yt_ref[...], preferred_element_type=f32)
        out_ref[0, :, h * PACK:(h + 1) * PACK, :] = r.reshape(chans, PACK, width).astype(bf16)

    keep_ref[...] = held_ref[...]
    cf[...] = co_ref[...].astype(f32).reshape(cf.shape)

    def outer(r, carry):
        total = cf[pl.ds(r, 1), :] * gm_ref[0, 0].astype(f32)
        for p in range(1, planes):
            total = total + cf[pl.ds(p * rows_here + r, 1), :] * gm_ref[p, 0].astype(f32)
        gs_ref[r] = total
        return carry

    lax.fori_loop(0, rows_here, outer, 0, unroll=4)


def backward_space(gp, g, table_y, kron, co, gm, held, parts):
    planes, chans, slab, cells = gp.shape
    groups, modes = g.shape[1], g.shape[2]
    own = co.shape[1]
    width = cells // parts
    rows_here = own * chans // (planes * parts)
    field = pl.BlockSpec((1, chans, slab, width), lambda p, h: (p, 0, 0, h))
    return pl.pallas_call(
        backward_kernel,
        grid=(planes, parts),
        out_shape=(
            jax.ShapeDtypeStruct(gp.shape, bf16),
            jax.ShapeDtypeStruct((own * chans, chans, modes), f32),
            jax.ShapeDtypeStruct(gp.shape, bf16),
        ),
        in_specs=[
            field,
            pl.BlockSpec((1, groups, modes, LANES), lambda p, h: (p, 0, 0, 0)),
            pl.BlockSpec((modes, width), lambda p, h: (0, h)),
            pl.BlockSpec(kron.shape, lambda p, h: (0, 0), pipeline_mode=pl.Buffered(1)),
            pl.BlockSpec((planes, rows_here, modes), lambda p, h: (0, p * parts + h, 0)),
            pl.BlockSpec((planes, 1, chans, modes), lambda p, h: (0, (p * parts + h) * rows_here // chans, 0, 0)),
            field,
        ],
        out_specs=(field, pl.BlockSpec((rows_here, chans, modes), lambda p, h: (p * parts + h, 0, 0)), field),
        scratch_shapes=[
            pltpu.VMEM((chans * PACK, width), bf16),
            pltpu.VMEM((slab // PACK, chans * PACK, modes), bf16),
            pltpu.VMEM((planes * rows_here, modes), f32),
        ],
        compiler_params=pltpu.CompilerParams(vmem_limit_bytes=56 << 20),
        name="backward_space",
    )(gp, g, table_y.T, kron, co.reshape(planes, own * chans, modes), gm, held)


def kernel_shards(nx, ny, flow_field, cotangent, spectral_weight, local_weight, channel_bias):
    planes, chans, slab, cells = flow_field.shape
    across = slab * nx * ny
    own, modes = spectral_weight.shape[0], spectral_weight.shape[3]
    scale_inv = math.sqrt(1.0 / (modes // 2))
    fwd_x = basis_table(across, modes, math.sqrt(2.0 / across))
    fwd_y = basis_table(cells, modes, math.sqrt(2.0 / cells))
    inv_x = basis_table(across, modes, scale_inv)
    inv_y = basis_table(cells, modes, scale_inv)
    out, grad_pre, back, kron, coeffs, grad_mixed = main_pass(
        nx, ny, flow_field, cotangent, spectral_weight, local_weight, channel_bias, fwd_y, inv_y, fwd_x, inv_x)
    grad_field, grad_spectral, out = backward_space(grad_pre, back, fwd_y, kron, coeffs, grad_mixed, out, 2)
    return out, grad_field, grad_spectral.reshape(own, chans, chans, modes)


def solution(mesh):
    nx, ny = mesh.shape["gx"], mesh.shape["gy"]

    def shards(flow_field, cotangent, spectral_weight, local_weight, channel_bias):
        planes, chans, slab, cells = flow_field.shape
        own, modes = spectral_weight.shape[0], spectral_weight.shape[3]
        fits = (
            slab % PACK == 0 and LANES % slab == 0 and modes == LANES
            and nx % 2 == 0 and (modes // nx) % PACK == 0
            and chans % (2 * LANES // slab) == 0 and chans % PACK == 0
            and cells % (2 * LANES) == 0
            and own * nx * ny == modes and chans % (own * chans // (2 * planes)) == 0
        )
        args = (flow_field, cotangent, spectral_weight, local_weight, channel_bias)
        return kernel_shards(nx, ny, *args) if fits else plain_shards(*args)

    placed = (
        P(None, None, ("gx", "gy"), None),
        P(None, None, ("gx", "gy"), None),
        P(("gx", "gy"), None, None, None),
        P(),
        P(),
    )
    return jax.shard_map(
        shards,
        mesh=mesh,
        in_specs=placed,
        out_specs=(
            P(None, None, ("gx", "gy"), None),
            P(None, None, ("gx", "gy"), None),
            P(("gx", "gy"), None, None, None),
        ),
        check_vma=False,
    )
```

```python
import functools
import math

import jax
import jax.numpy as jnp
import numpy as np
from jax import lax
from jax.experimental import pallas as pl
from jax.experimental.pallas import tpu as pltpu
from jax.sharding import PartitionSpec as P

root_half = 0.7071067811865476
density_norm = 0.3989422804014327
LANES = 128
PACK = 16
MESH = pl.DeviceIdType.MESH
f32, bf16 = jnp.float32, jnp.bfloat16


def basis_table(cells, cols, factor):
    kept = cols // 2
    columns = np.arange(cols)
    frequency = np.where(columns < kept, columns, columns - kept + 1)
    phases = np.arange(cells)[:, None] * frequency[None, :] % cells
    angles = phases.astype(np.float32) * np.float32(2.0 * math.pi / cells)
    values = np.where(columns[None, :] < kept, np.cos(angles), np.sin(angles))
    return jnp.asarray((values * np.float32(factor)).astype(jnp.bfloat16))


def gelu_slope(values):
    cumulative = 0.5 * (1.0 + lax.erf(values * root_half))
    density = jnp.exp(-0.5 * values * values) * density_norm
    return cumulative + values * density


def dot_t(a, b, da, db):
    return lax.dot_general(a, b, (((da,), (db,)), ((), ())), preferred_element_type=f32)


def to_owners(modal_rows):
    return lax.all_to_all(modal_rows, ("gx", "gy"), split_axis=0, concat_axis=1, tiled=True)


def to_slabs(modal_part):
    return lax.all_to_all(modal_part, ("gx", "gy"), split_axis=1, concat_axis=0, tiled=True)


def contract(spec, left, right):
    return jnp.einsum(spec, left, right, preferred_element_type=jnp.float32)


def plain_shards(flow_field, cotangent, spectral_weight, local_weight, channel_bias):
    devices = lax.axis_size("gx") * lax.axis_size("gy")
    planes, channels, slab_rows, cells_along = flow_field.shape
    cells_across = slab_rows * devices
    own_cols = spectral_weight.shape[0]
    mode_cols = spectral_weight.shape[3]
    kept_modes = mode_cols // 2
    both = planes * channels
    scale_inv = math.sqrt(1.0 / kept_modes)
    fwd_x = basis_table(cells_across, mode_cols, math.sqrt(2.0 / cells_across))
    fwd_y = basis_table(cells_along, mode_cols, math.sqrt(2.0 / cells_along))
    inv_x = basis_table(cells_across, mode_cols, scale_inv)
    inv_y = basis_table(cells_along, mode_cols, scale_inv)

    def to_modes(field, table_x, table_y):
        rows = contract("axy,yj->jxa", field.reshape(both, slab_rows, cells_along), table_y)
        received = to_owners(rows.astype(jnp.bfloat16))
        modes = contract("jxa,xk->jka", received, table_x).astype(jnp.bfloat16)
        return modes.reshape(own_cols, mode_cols, planes, channels)

    def to_rows(modes, table_x):
        merged = modes.reshape(own_cols, mode_cols, both)
        return to_slabs(contract("jka,xk->jxa", merged, table_x).astype(jnp.bfloat16))

    def to_space(rows, table_y):
        field = contract("jxa,yj->axy", rows, table_y)
        return field.reshape(planes, channels, slab_rows, cells_along)

    coeffs = to_modes(flow_field, fwd_x, fwd_y)
    mixed = contract("jkzi,jiok->jkzo", coeffs, spectral_weight).astype(jnp.bfloat16)
    gathered = to_rows(mixed, inv_x)
    spectral = to_space(gathered, inv_y)
    pointwise = contract("zixy,io->zoxy", flow_field, local_weight)
    pre_activation = spectral + pointwise + channel_bias[None, :, None, None]
    output_field = jax.nn.gelu(pre_activation, approximate=False).astype(jnp.bfloat16)
    grad_pre = (cotangent.astype(jnp.float32) * gelu_slope(pre_activation)).astype(jnp.bfloat16)
    grad_mixed = to_modes(grad_pre, inv_x, inv_y)
    grad_coeffs = contract("jkzo,jiok->jkzi", grad_mixed, spectral_weight).astype(jnp.bfloat16)
    gathered_back = to_rows(grad_coeffs, fwd_x)
    grad_spectral = contract("jkzi,jkzo->jiok", coeffs, grad_mixed)
    backward = to_space(gathered_back, fwd_y)
    through_local = contract("zoxy,io->zixy", grad_pre, local_weight)
    grad_field = (backward + through_local).astype(jnp.bfloat16)
    return (output_field, grad_field, grad_spectral)


def main_kernel(
    nx, ny, planes, chans, slab, modes, own,
    flow_hbm, cot_hbm, w_hbm, lw_ref, bias_ref, fy_ref, iy_ref, fx_ref, ix_ref,
    cbuf, fbuf, back_ref, co_ref, gm_ref,
    wbuf, tx, kron, kron_t, sbuf, rbuf, part, zs, zr, cf, gf, ms, zg, tg, lhs2, isb,
    gbuf, gt, pre, xs,
    load_sem, cot_sem, w_sem, s1, r1, s2, r2, s3, r3, s4, r4,
):
    gx, gy = lax.axis_index("gx"), lax.axis_index("gy")
    per = LANES // slab
    groups = chans // per
    jg = modes // nx
    cells = fbuf.shape[3]
    halves = slab // PACK
    width = 2 * LANES
    parts = cells // width

    def load(p):
        return pltpu.make_async_copy(flow_hbm.at[p], fbuf.at[p], load_sem.at[p])

    def load_cot(p):
        return pltpu.make_async_copy(cot_hbm.at[p], cbuf.at[p], cot_sem.at[p])

    def load_w():
        return pltpu.make_async_copy(w_hbm, wbuf, w_sem)

    for p in range(planes):
        load(p).start()
    load_w().start()
    for p in range(planes):
        load_cot(p).start()

    barrier = pltpu.get_barrier_semaphore()
    for o in range(1, nx):
        pl.semaphore_signal(barrier, inc=1, device_id=((gx + o) % nx, gy), device_id_type=MESH)
    for o in range(1, ny):
        pl.semaphore_signal(barrier, inc=1, device_id=(gx, (gy + o) % ny), device_id_type=MESH)

    def lane(g):
        return pl.ds(pl.multiple_of(g * LANES, LANES), LANES)

    def jrows(g):
        return pl.ds(pl.multiple_of(g * jg, jg), jg)

    def rows(f, p, o, out):
        other = (gx + o) % nx if out else (gx + nx - o) % nx
        slot = gx if out else other
        return pltpu.make_async_remote_copy(
            sbuf.at[f, p, other], rbuf.at[f, p, :, :, lane(slot)], s1.at[f, p, o], r1.at[f, p, o],
            device_id=(other, gy), device_id_type=MESH)

    def sums(f, p, o, out):
        other = (gy + o) % ny if out else (gy + ny - o) % ny
        slot = gy if out else other
        return pltpu.make_async_remote_copy(
            zs.at[f, p, other], zr.at[f, p, slot], s2.at[f, p, o], r2.at[f, p, o],
            device_id=(gx, other), device_id_type=MESH)

    def mixed(f, p, o, out):
        other = (gy + o) % ny if out else (gy + ny - o) % ny
        slot = gy if out else other
        return pltpu.make_async_remote_copy(
            ms.at[f, p], zg.at[f, p, slot], s3.at[f, p, o], r3.at[f, p, o],
            device_id=(gx, other), device_id_type=MESH)

    def back(f, p, o, out):
        other = (gx + o) % nx if out else (gx + nx - o) % nx
        slot = gx if out else other
        into = back_ref if f else gbuf
        return pltpu.make_async_remote_copy(
            isb.at[f, p, other], into.at[p, :, jrows(slot), :], s4.at[f, p, o], r4.at[f, p, o],
            device_id=(other, gy), device_id_type=MESH)

    def analyse(f, p):
        table = iy_ref if f else fy_ref

        def body(t, carry):
            x = fbuf[p, pl.ds(t * 2 * per, 2 * per)].reshape(2 * LANES, cells)
            r = dot_t(table[...], x, 1, 1).astype(bf16)
            for h in range(2):
                sbuf[f, p, :, t * 2 + h] = r[:, h * LANES:(h + 1) * LANES].reshape(nx, jg, LANES)
            return carry

        lax.fori_loop(0, groups // 2, body, 0, unroll=2)
        rbuf[f, p, :, :, lane(gx)] = sbuf[f, p, gx]

    def send_rows(f, p):
        for o in range(1, nx):
            rows(f, p, o, True).start()

    def across(f, p):
        for o in range(1, nx):
            rows(f, p, o, False).wait_recv()
        left = rbuf[f, p].reshape(groups * jg, nx * LANES)
        r = jnp.dot(left, tx[f], preferred_element_type=f32)
        for g in range(groups):
            for c in range(per):
                part[pl.ds((g * per + c) * jg, jg), :] = r[g * jg:(g + 1) * jg, c * modes:(c + 1) * modes]
        for j in range(jg):
            zs[f, p, j // own, j % own] = part[pl.ds(j, chans, stride=jg), :].astype(bf16)
        zr[f, p, gy] = zs[f, p, gy]
        for o in range(1, ny):
            sums(f, p, o, True).start()

    def mix(f, p):
        for o in range(1, ny):
            sums(f, p, o, False).wait_recv()
        total = zr[f, p, 0].astype(f32)
        for s in range(1, ny):
            total = total + zr[f, p, s].astype(f32)
        coef = total.astype(bf16)
        if f:
            gm_ref[p] = coef
        else:
            co_ref[p] = coef
        cf[...] = coef.astype(f32).reshape(own * chans, modes)
        for j in range(own):
            if f:
                right = cf[pl.ds(j * chans, chans), :]

                def body(i, carry):
                    prod = wbuf[j, i].astype(f32) * right
                    gf[pl.ds(i, 1), :] = jnp.sum(prod, axis=0, keepdims=True)
                    return carry

                lax.fori_loop(0, chans, body, 0, unroll=8)
                ms[f, p, j] = gf[...].astype(bf16)
            else:

                def body(i, acc):
                    return acc + cf[pl.ds(j * chans + i, 1), :] * wbuf[j, i].astype(f32)

                acc = lax.fori_loop(0, chans, body, jnp.zeros((chans, modes), f32), unroll=8)
                ms[f, p, j] = acc.astype(bf16)
        zg[f, p, gy] = ms[f, p]
        for o in range(1, ny):
            mixed(f, p, o, True).start()

    def expand(f, p):
        for o in range(1, ny):
            mixed(f, p, o, False).wait_recv()
        tg[...] = zg[f, p].astype(f32).reshape(ny * own * chans, modes)
        for c in range(chans):
            lhs2[pl.ds((c // per) * jg, jg), pl.ds((c % per) * modes, modes)] = tg[pl.ds(c, jg, stride=chans), :].astype(bf16)

        def body(t, carry):
            table = tx[1 - f, pl.ds(pl.multiple_of(t * 2 * LANES, LANES), 2 * LANES), :]
            r = dot_t(lhs2[...], table, 1, 1).astype(bf16)
            for h in range(2):
                isb[f, p, t * 2 + h] = r[:, h * LANES:(h + 1) * LANES].reshape(groups, jg, LANES)
            return carry

        lax.fori_loop(0, nx // 2, body, 0, unroll=2)
        into = back_ref if f else gbuf
        into[p, :, jrows(gx), :] = isb[f, p, gx]
        for o in range(1, nx):
            back(f, p, o, True).start()

    def point(p):
        load_cot(p).wait()
        for o in range(1, nx):
            back(0, p, o, False).wait_recv()

        def turn(g, carry):
            block = gbuf[p, g].T.reshape(per, halves, PACK, modes)
            for h in range(halves):
                gt[h, pl.ds(g * per * PACK, per * PACK), :] = block[:, h].reshape(per * PACK, modes)
            return carry

        lax.fori_loop(0, groups, turn, 0, unroll=4)

        def piece(s, carry):
            h, y = s // parts, s % parts
            rows16 = pl.ds(pl.multiple_of(h * PACK, PACK), PACK)
            cols = pl.ds(pl.multiple_of(y * width, width), width)
            xs[...] = fbuf[p, :, rows16, cols].reshape(chans * PACK, width)
            r = jnp.dot(kron[...], xs[...], preferred_element_type=f32)
            r = r + jnp.dot(gt[h], iy_ref[:, cols], preferred_element_type=f32)
            pre[...] = r.reshape(chans, PACK, width)

            def one(c, inner):
                v = pre[c] + bias_ref[c]
                phi = 0.5 + 0.5 * lax.erf(v * root_half)
                density = jnp.exp(-0.5 * v * v) * density_norm
                cot = cbuf[p, c, rows16, cols].astype(f32)
                cbuf[p, c, rows16, cols] = (v * phi).astype(bf16)
                fbuf[p, c, rows16, cols] = (cot * (phi + v * density)).astype(bf16)
                return inner

            lax.fori_loop(0, chans, one, 0, unroll=4)
            return carry

        lax.fori_loop(0, halves * parts, piece, 0)

    def through(p):
        def piece(s, carry):
            h, y = s // parts, s % parts
            rows16 = pl.ds(pl.multiple_of(h * PACK, PACK), PACK)
            cols = pl.ds(pl.multiple_of(y * width, width), width)
            xs[...] = fbuf[p, :, rows16, cols].reshape(chans * PACK, width)
            r = jnp.dot(kron_t[...], xs[...], preferred_element_type=f32)
            fbuf[p, :, rows16, cols] = r.astype(bf16).reshape(chans, PACK, width)
            return carry

        lax.fori_loop(0, halves * parts, piece, 0)

    load(0).wait()
    analyse(0, 0)
    pl.semaphore_wait(barrier, nx + ny - 2)
    send_rows(0, 0)

    def first(p, carry):
        load(p).wait()
        analyse(0, p)
        send_rows(0, p)
        return carry

    lax.fori_loop(1, planes, first, 0)

    tx[...] = jnp.zeros_like(tx)
    for f, ref in enumerate((fx_ref, ix_ref)):
        for s in range(nx):
            for c in range(per):
                tx[f, pl.ds(s * LANES + c * slab, slab), pl.ds(c * modes, modes)] = ref[s, gy]

    tall = chans * PACK
    row = lax.broadcasted_iota(jnp.int32, (tall, chans), 0) // PACK
    col = lax.broadcasted_iota(jnp.int32, (tall, chans), 1)
    pick = jnp.where(row == col, 1.0, 0.0).astype(bf16)
    right = dot_t(lw_ref[...], pick, 1, 1).astype(bf16)
    left = dot_t(lw_ref[...], pick, 0, 1).astype(bf16)
    cut = 2 * LANES
    for k in range(tall // cut):
        sub = pick[k * cut:(k + 1) * cut]
        keep = (lax.broadcasted_iota(jnp.int32, (cut, tall), 0) % PACK
                == lax.broadcasted_iota(jnp.int32, (cut, tall), 1) % PACK)
        rows_k = pl.ds(k * cut, cut)
        kron_t[rows_k, :] = jnp.where(keep, jnp.dot(sub, right, preferred_element_type=f32), 0.0).astype(bf16)
        kron[rows_k, :] = jnp.where(keep, jnp.dot(sub, left, preferred_element_type=f32), 0.0).astype(bf16)
    load_w().wait()

    def step(t, carry):
        def stage(lag, run):
            @pl.when((t >= lag) & (t < planes + lag))
            def _():
                run(t - lag)

        def middle(p):
            point(p)
            analyse(1, p)
            send_rows(1, p)

        stage(0, functools.partial(across, 0))
        stage(1, functools.partial(mix, 0))
        stage(2, functools.partial(expand, 0))
        stage(3, middle)
        stage(4, functools.partial(across, 1))
        stage(5, functools.partial(mix, 1))
        stage(6, functools.partial(expand, 1))
        stage(6, through)
        return carry

    lax.fori_loop(0, planes + 6, step, 0)

    def finish(p, carry):
        for f in range(2):
            for o in range(1, nx):
                rows(f, p, o, True).wait_send()
                back(f, p, o, True).wait_send()
            for o in range(1, ny):
                sums(f, p, o, True).wait_send()
                mixed(f, p, o, True).wait_send()
        for o in range(1, nx):
            back(1, p, o, False).wait_recv()
        return carry

    lax.fori_loop(0, planes, finish, 0)


def main_pass(nx, ny, flow, cot, weight, local_weight, bias, fwd_y, inv_y, fwd_x, inv_x):
    planes, chans, slab, cells = flow.shape
    own, modes = weight.shape[0], weight.shape[3]
    per = LANES // slab
    groups = chans // per
    jg = modes // nx
    tall = chans * PACK
    vm = pl.BlockSpec(memory_space=pltpu.VMEM)
    hbm = pl.BlockSpec(memory_space=pl.ANY)
    dma = pltpu.SemaphoreType.DMA
    split = lambda t: t.reshape(nx, ny, slab, modes)
    field = pltpu.VMEM(flow.shape, bf16)
    coef = pltpu.VMEM((planes, own, chans, modes), bf16)
    return pl.pallas_call(
        functools.partial(main_kernel, nx, ny, planes, chans, slab, modes, own),
        out_shape=(
            field, field,
            pltpu.VMEM((planes, groups, modes, LANES), bf16),
            coef, coef,
        ),
        in_specs=[hbm, hbm, hbm, vm, pl.BlockSpec(memory_space=pltpu.SMEM), vm, vm, vm, vm],
        out_specs=(vm, vm, vm, vm, vm),
        scratch_shapes=[
            pltpu.VMEM(weight.shape, bf16),
            pltpu.VMEM((2, nx * LANES, per * modes), bf16),
            pltpu.VMEM((tall, tall), bf16),
            pltpu.VMEM((tall, tall), bf16),
            pltpu.VMEM((2, planes, nx, groups, jg, LANES), bf16),
            pltpu.VMEM((2, planes, groups, jg, nx * LANES), bf16),
            pltpu.VMEM((chans * jg, modes), f32),
            pltpu.VMEM((2, planes, ny, own, chans, modes), bf16),
            pltpu.VMEM((2, planes, ny, own, chans, modes), bf16),
            pltpu.VMEM((own * chans, modes), f32),
            pltpu.VMEM((chans, modes), f32),
            pltpu.VMEM((2, planes, own, chans, modes), bf16),
            pltpu.VMEM((2, planes, ny, own, chans, modes), bf16),
            pltpu.VMEM((ny * own * chans, modes), f32),
            pltpu.VMEM((groups * jg, per * modes), bf16),
            pltpu.VMEM((2, planes, nx, groups, jg, LANES), bf16),
            pltpu.VMEM((planes, groups, modes, LANES), bf16),
            pltpu.VMEM((slab // PACK, tall, modes), bf16),
            pltpu.VMEM((chans, PACK, 2 * LANES), f32),
            pltpu.VMEM((tall, 2 * LANES), bf16),
            dma((planes,)), dma((planes,)), dma,
            dma((2, planes, nx)), dma((2, planes, nx)),
            dma((2, planes, ny)), dma((2, planes, ny)),
            dma((2, planes, ny)), dma((2, planes, ny)),
            dma((2, planes, nx)), dma((2, planes, nx)),
        ],
        compiler_params=pltpu.CompilerParams(
            collective_id=0, has_side_effects=True, vmem_limit_bytes=40 << 20),
        name="main_pass",
    )(flow, cot, weight, local_weight, bias, fwd_y.T, inv_y.T, split(fwd_x), split(inv_x))


def rows_by_half(g_ref, p, gt):
    groups = g_ref.shape[1]
    halves, tall, modes = gt.shape
    slab = halves * PACK
    per = LANES // slab

    def turn(g, carry):
        block = g_ref[p, g].T.reshape(per, halves, PACK, modes)
        for h in range(halves):
            gt[h, pl.ds(g * per * PACK, per * PACK), :] = block[:, h].reshape(per * PACK, modes)
        return carry

    lax.fori_loop(0, groups, turn, 0, unroll=4)


def last_kernel(thru_ref, g_ref, yt_ref, co_ref, gm_ref, held_ref, out_ref, gs_ref, keep_hbm, gt, cf, sem):
    _, chans, slab, width = out_ref.shape
    planes, own = co_ref.shape[:2]
    rows_here = gs_ref.shape[0]
    p, part = pl.program_id(0), pl.program_id(1)

    def keep(q):
        return pltpu.make_async_copy(held_ref.at[q], keep_hbm.at[q], sem.at[q])

    @pl.when(part == 0)
    def _():
        keep(p).start()
        rows_by_half(g_ref, p, gt)

    cols = pl.ds(pl.multiple_of(part * width, width), width)
    for h in range(slab // PACK):
        r = jnp.dot(gt[h], yt_ref[...], preferred_element_type=f32).reshape(chans, PACK, width)
        r = r + thru_ref[p, :, h * PACK:(h + 1) * PACK, cols].astype(f32)
        out_ref[0, :, h * PACK:(h + 1) * PACK, :] = r.astype(bf16)

    first = (p * pl.num_programs(1) + part) * rows_here
    j, i = first // chans, pl.multiple_of(first % chans, rows_here)
    cf[...] = co_ref[:, j, pl.ds(i, rows_here), :].astype(f32).reshape(cf.shape)

    def outer(r, carry):
        total = cf[pl.ds(r, 1), :] * gm_ref[0, j].astype(f32)
        for q in range(1, planes):
            total = total + cf[pl.ds(q * rows_here + r, 1), :] * gm_ref[q, j].astype(f32)
        gs_ref[r] = total
        return carry

    lax.fori_loop(0, rows_here, outer, 0, unroll=4)

    @pl.when((p == planes - 1) & (part == pl.num_programs(1) - 1))
    def _():
        for q in range(planes):
            keep(q).wait()


def last_pass(thru, g, table_y, co, gm, held, parts):
    planes, chans, slab, cells = thru.shape
    modes, own = g.shape[2], co.shape[1]
    width = cells // parts
    rows_here = own * chans // (planes * parts)
    field = pl.BlockSpec((1, chans, slab, width), lambda p, h: (p, 0, 0, h))
    whole = pl.BlockSpec(memory_space=pltpu.VMEM)
    shape = jax.ShapeDtypeStruct(thru.shape, bf16)
    return pl.pallas_call(
        last_kernel,
        grid=(planes, parts),
        out_shape=(shape, jax.ShapeDtypeStruct((own * chans, chans, modes), f32), shape),
        in_specs=[
            whole,
            whole,
            pl.BlockSpec((modes, width), lambda p, h: (0, h)),
            whole, whole, whole,
        ],
        out_specs=(
            field,
            pl.BlockSpec((rows_here, chans, modes), lambda p, h: (p * parts + h, 0, 0)),
            pl.BlockSpec(memory_space=pl.ANY),
        ),
        scratch_shapes=[
            pltpu.VMEM((slab // PACK, chans * PACK, modes), bf16),
            pltpu.VMEM((planes * rows_here, modes), f32),
            pltpu.SemaphoreType.DMA((planes,)),
        ],
        compiler_params=pltpu.CompilerParams(vmem_limit_bytes=20 << 20),
        name="last_pass",
    )(thru, g, table_y.T, co, gm, held)


def kernel_shards(nx, ny, flow_field, cotangent, spectral_weight, local_weight, channel_bias):
    planes, chans, slab, cells = flow_field.shape
    across = slab * nx * ny
    own, modes = spectral_weight.shape[0], spectral_weight.shape[3]
    scale_inv = math.sqrt(1.0 / (modes // 2))
    fwd_x = basis_table(across, modes, math.sqrt(2.0 / across))
    fwd_y = basis_table(cells, modes, math.sqrt(2.0 / cells))
    inv_x = basis_table(across, modes, scale_inv)
    inv_y = basis_table(cells, modes, scale_inv)
    out, thru, back, coeffs, grad_mixed = main_pass(
        nx, ny, flow_field, cotangent, spectral_weight, local_weight, channel_bias, fwd_y, inv_y, fwd_x, inv_x)
    grad_field, grad_spectral, out = last_pass(thru, back, fwd_y, coeffs, grad_mixed, out, 2)
    return out, grad_field, grad_spectral.reshape(own, chans, chans, modes)


def solution(mesh):
    nx, ny = mesh.shape["gx"], mesh.shape["gy"]

    def shards(flow_field, cotangent, spectral_weight, local_weight, channel_bias):
        planes, chans, slab, cells = flow_field.shape
        own, modes = spectral_weight.shape[0], spectral_weight.shape[3]
        fits = (
            slab % PACK == 0 and LANES % slab == 0 and modes == LANES
            and nx % 2 == 0 and (modes // nx) % PACK == 0
            and chans % (2 * LANES // slab) == 0 and chans % PACK == 0
            and cells % (2 * LANES) == 0
            and own * nx * ny == modes and chans % (own * chans // (2 * planes)) == 0
        )
        args = (flow_field, cotangent, spectral_weight, local_weight, channel_bias)
        return kernel_shards(nx, ny, *args) if fits else plain_shards(*args)

    placed = (
        P(None, None, ("gx", "gy"), None),
        P(None, None, ("gx", "gy"), None),
        P(("gx", "gy"), None, None, None),
        P(),
        P(),
    )
    return jax.shard_map(
        shards,
        mesh=mesh,
        in_specs=placed,
        out_specs=(
            P(None, None, ("gx", "gy"), None),
            P(None, None, ("gx", "gy"), None),
            P(("gx", "gy"), None, None, None),
        ),
        check_vma=False,
    )
```

```python
import functools
import math

import jax
import jax.numpy as jnp
import numpy as np
from jax import lax
from jax.experimental import pallas as pl
from jax.experimental.pallas import tpu as pltpu
from jax.sharding import PartitionSpec as P

root_half = 0.7071067811865476
density_norm = 0.3989422804014327
LANES = 128
PACK = 16
MESH = pl.DeviceIdType.MESH
f32, bf16 = jnp.float32, jnp.bfloat16


def basis_table(cells, cols, factor):
    kept = cols // 2
    columns = np.arange(cols)
    frequency = np.where(columns < kept, columns, columns - kept + 1)
    phases = np.arange(cells)[:, None] * frequency[None, :] % cells
    angles = phases.astype(np.float32) * np.float32(2.0 * math.pi / cells)
    values = np.where(columns[None, :] < kept, np.cos(angles), np.sin(angles))
    return jnp.asarray((values * np.float32(factor)).astype(jnp.bfloat16))


def gelu_slope(values):
    cumulative = 0.5 * (1.0 + lax.erf(values * root_half))
    density = jnp.exp(-0.5 * values * values) * density_norm
    return cumulative + values * density


def dot_t(a, b, da, db):
    return lax.dot_general(a, b, (((da,), (db,)), ((), ())), preferred_element_type=f32)


def to_owners(modal_rows):
    return lax.all_to_all(modal_rows, ("gx", "gy"), split_axis=0, concat_axis=1, tiled=True)


def to_slabs(modal_part):
    return lax.all_to_all(modal_part, ("gx", "gy"), split_axis=1, concat_axis=0, tiled=True)


def contract(spec, left, right):
    return jnp.einsum(spec, left, right, preferred_element_type=jnp.float32)


def plain_shards(flow_field, cotangent, spectral_weight, local_weight, channel_bias):
    devices = lax.axis_size("gx") * lax.axis_size("gy")
    planes, channels, slab_rows, cells_along = flow_field.shape
    cells_across = slab_rows * devices
    own_cols = spectral_weight.shape[0]
    mode_cols = spectral_weight.shape[3]
    kept_modes = mode_cols // 2
    both = planes * channels
    scale_inv = math.sqrt(1.0 / kept_modes)
    fwd_x = basis_table(cells_across, mode_cols, math.sqrt(2.0 / cells_across))
    fwd_y = basis_table(cells_along, mode_cols, math.sqrt(2.0 / cells_along))
    inv_x = basis_table(cells_across, mode_cols, scale_inv)
    inv_y = basis_table(cells_along, mode_cols, scale_inv)

    def to_modes(field, table_x, table_y):
        rows = contract("axy,yj->jxa", field.reshape(both, slab_rows, cells_along), table_y)
        received = to_owners(rows.astype(jnp.bfloat16))
        modes = contract("jxa,xk->jka", received, table_x).astype(jnp.bfloat16)
        return modes.reshape(own_cols, mode_cols, planes, channels)

    def to_rows(modes, table_x):
        merged = modes.reshape(own_cols, mode_cols, both)
        return to_slabs(contract("jka,xk->jxa", merged, table_x).astype(jnp.bfloat16))

    def to_space(rows, table_y):
        field = contract("jxa,yj->axy", rows, table_y)
        return field.reshape(planes, channels, slab_rows, cells_along)

    coeffs = to_modes(flow_field, fwd_x, fwd_y)
    mixed = contract("jkzi,jiok->jkzo", coeffs, spectral_weight).astype(jnp.bfloat16)
    gathered = to_rows(mixed, inv_x)
    spectral = to_space(gathered, inv_y)
    pointwise = contract("zixy,io->zoxy", flow_field, local_weight)
    pre_activation = spectral + pointwise + channel_bias[None, :, None, None]
    output_field = jax.nn.gelu(pre_activation, approximate=False).astype(jnp.bfloat16)
    grad_pre = (cotangent.astype(jnp.float32) * gelu_slope(pre_activation)).astype(jnp.bfloat16)
    grad_mixed = to_modes(grad_pre, inv_x, inv_y)
    grad_coeffs = contract("jkzo,jiok->jkzi", grad_mixed, spectral_weight).astype(jnp.bfloat16)
    gathered_back = to_rows(grad_coeffs, fwd_x)
    grad_spectral = contract("jkzi,jkzo->jiok", coeffs, grad_mixed)
    backward = to_space(gathered_back, fwd_y)
    through_local = contract("zoxy,io->zixy", grad_pre, local_weight)
    grad_field = (backward + through_local).astype(jnp.bfloat16)
    return (output_field, grad_field, grad_spectral)


def main_kernel(
    nx, ny, planes, chans, slab, modes, own,
    flow_hbm, cot_hbm, w_hbm, lw_ref, bias_ref, fy_ref, iy_ref, fx_ref, ix_ref,
    cbuf, fbuf, back_ref, co_ref, gm_ref,
    wbuf, tx, kron, kron_t, sbuf, rbuf, part, zs, zr, zq, cf, ms, zg, tg, lhs2, isb,
    gbuf, gt, pre, xs,
    load_sem, cot_sem, w_sem, s1, r1, s2, r2, s3, r3, s4, r4,
):
    gx, gy = lax.axis_index("gx"), lax.axis_index("gy")
    per = LANES // slab
    groups = chans // per
    jg = modes // nx
    cells = fbuf.shape[3]
    halves = slab // PACK
    width = 2 * LANES
    parts = cells // width

    def load(p):
        return pltpu.make_async_copy(flow_hbm.at[p], fbuf.at[p], load_sem.at[p])

    def load_cot(p):
        return pltpu.make_async_copy(cot_hbm.at[p], cbuf.at[p], cot_sem.at[p])

    def load_w():
        return pltpu.make_async_copy(w_hbm, wbuf, w_sem)

    for p in range(planes):
        load(p).start()
    load_w().start()
    for p in range(planes):
        load_cot(p).start()

    barrier = pltpu.get_barrier_semaphore()
    for o in range(1, nx):
        pl.semaphore_signal(barrier, inc=1, device_id=((gx + o) % nx, gy), device_id_type=MESH)
    for o in range(1, ny):
        pl.semaphore_signal(barrier, inc=1, device_id=(gx, (gy + o) % ny), device_id_type=MESH)

    def lane(g):
        return pl.ds(pl.multiple_of(g * LANES, LANES), LANES)

    def jrows(g):
        return pl.ds(pl.multiple_of(g * jg, jg), jg)

    def rows(f, p, o, out):
        other = (gx + o) % nx if out else (gx + nx - o) % nx
        slot = gx if out else other
        return pltpu.make_async_remote_copy(
            sbuf.at[f, p, other], rbuf.at[f, p, :, :, lane(slot)], s1.at[f, p, o], r1.at[f, p, o],
            device_id=(other, gy), device_id_type=MESH)

    side = gy // 2
    outer, inner = 3 * side, 1 + side
    far_inner, far_outer = 2 - side, 3 - 3 * side
    partner = outer + inner - gy
    at_inner = gy == inner
    at_outer = gy != inner

    def along(f, p, src, dst, to, sent, got):
        return pltpu.make_async_remote_copy(
            src, dst, sent, got, device_id=(gx, to), device_id_type=MESH)

    def sums_near(f, p, i, dest, to):
        return along(f, p, zs.at[f, p, dest], zr.at[f, p, i], to, s2.at[f, p, i], r2.at[f, p, i])

    def sums_far(f, p, i, to):
        return along(f, p, zq.at[f, p, i], zr.at[f, p, 3], to, s2.at[f, p, 1 + i], r2.at[f, p, 3])

    def mixed_near(f, p, i, slot, to):
        return along(f, p, ms.at[f, p], zg.at[f, p, slot], to, s3.at[f, p, i], r3.at[f, p, slot])

    def mixed_on(f, p, i, slot, to):
        return along(f, p, zg.at[f, p, slot], zg.at[f, p, slot], to, s3.at[f, p, 2 + i], r3.at[f, p, slot])

    def send_sums(f, p):
        @pl.when(at_outer)
        def _():
            for i, dest in enumerate((inner, far_inner, far_outer)):
                sums_near(f, p, i, dest, inner).start()

        @pl.when(at_inner)
        def _():
            sums_near(f, p, 0, outer, outer).start()

    def relay_sums(f, p):
        @pl.when(at_inner)
        def _():
            for i in range(3):
                sums_near(f, p, i, gy, outer).wait_recv()
            for i, dest in enumerate((far_inner, far_outer)):
                zq[f, p, i] = (zr[f, p, 1 + i].astype(f32) + zs[f, p, dest].astype(f32)).astype(bf16)
                sums_far(f, p, i, dest).start()

    def take_sums(f, p):
        @pl.when(at_outer)
        def _():
            sums_near(f, p, 0, gy, inner).wait_recv()

        sums_far(f, p, 0, far_inner).wait_recv()
        return zs[f, p, gy].astype(f32) + zr[f, p, 0].astype(f32) + zr[f, p, 3].astype(f32)

    def send_mixed(f, p):
        mixed_near(f, p, 0, gy, partner).start()
        mixed_near(f, p, 1, gy, far_inner).start()

    def relay_mixed(f, p):
        @pl.when(at_inner)
        def _():
            for i, slot in enumerate((far_inner, far_outer)):
                mixed_near(f, p, i, slot, slot).wait_recv()
                mixed_on(f, p, i, slot, outer).start()

    def take_mixed(f, p):
        mixed_near(f, p, 0, partner, partner).wait_recv()

        @pl.when(at_outer)
        def _():
            for i, slot in enumerate((far_inner, far_outer)):
                mixed_on(f, p, i, slot, inner).wait_recv()

    def gy_sent(f, p):
        @pl.when(at_outer)
        def _():
            for i, dest in enumerate((inner, far_inner, far_outer)):
                sums_near(f, p, i, dest, inner).wait_send()

        @pl.when(at_inner)
        def _():
            sums_near(f, p, 0, outer, outer).wait_send()
            for i, dest in enumerate((far_inner, far_outer)):
                sums_far(f, p, i, dest).wait_send()
                mixed_on(f, p, i, dest, outer).wait_send()

        mixed_near(f, p, 0, gy, partner).wait_send()
        mixed_near(f, p, 1, gy, far_inner).wait_send()

    def back(f, p, o, out):
        other = (gx + o) % nx if out else (gx + nx - o) % nx
        slot = gx if out else other
        into = back_ref if f else gbuf
        return pltpu.make_async_remote_copy(
            isb.at[f, p, other], into.at[p, :, jrows(slot), :], s4.at[f, p, o], r4.at[f, p, o],
            device_id=(other, gy), device_id_type=MESH)

    def analyse(f, p):
        table = iy_ref if f else fy_ref

        wide = groups // 2

        def body(t, carry):
            x = fbuf[p, pl.ds(t * wide * per, wide * per)].reshape(wide * LANES, cells)
            r = dot_t(table[...], x, 1, 1).astype(bf16)
            for h in range(wide):
                sbuf[f, p, :, t * wide + h] = r[:, h * LANES:(h + 1) * LANES].reshape(nx, jg, LANES)
            return carry

        lax.fori_loop(0, 2, body, 0)
        rbuf[f, p, :, :, lane(gx)] = sbuf[f, p, gx]

    def send_rows(f, p):
        for o in range(1, nx):
            rows(f, p, o, True).start()

    def across(f, p):
        for o in range(1, nx):
            rows(f, p, o, False).wait_recv()
        left = rbuf[f, p].reshape(groups * jg, nx * LANES)
        r = jnp.dot(left, tx[f], preferred_element_type=f32)
        for g in range(groups):
            for c in range(per):
                part[pl.ds((g * per + c) * jg, jg), :] = r[g * jg:(g + 1) * jg, c * modes:(c + 1) * modes]
        for j in range(jg):
            zs[f, p, j // own, j % own] = part[pl.ds(j, chans, stride=jg), :].astype(bf16)
        send_sums(f, p)

    def mix(f, p):
        coef = take_sums(f, p).astype(bf16)
        if f:
            gm_ref[p] = coef
        else:
            co_ref[p] = coef
        cf[...] = coef.astype(f32).reshape(own * chans, modes)
        for j in range(own):
            if f:
                right = cf[pl.ds(j * chans, chans), :]

                def body(i, carry):
                    prod = wbuf[j, i].astype(f32) * right
                    part[pl.ds(pl.multiple_of(i * 8, 8), 8), :] = jnp.sum(prod.reshape(chans // 8, 8, modes), axis=0)
                    return carry

                lax.fori_loop(0, chans, body, 0, unroll=8)
                total = part[pl.ds(0, chans, stride=8), :]
                for k in range(1, 8):
                    total = total + part[pl.ds(k, chans, stride=8), :]
                ms[f, p, j] = total.astype(bf16)
            else:

                def body(i, acc):
                    return acc + cf[pl.ds(j * chans + i, 1), :] * wbuf[j, i].astype(f32)

                acc = lax.fori_loop(0, chans, body, jnp.zeros((chans, modes), f32), unroll=8)
                ms[f, p, j] = acc.astype(bf16)
        zg[f, p, gy] = ms[f, p]
        send_mixed(f, p)

    def expand(f, p):
        take_mixed(f, p)
        tg[...] = zg[f, p].astype(f32).reshape(ny * own * chans, modes)
        for c in range(chans):
            lhs2[pl.ds((c // per) * jg, jg), pl.ds((c % per) * modes, modes)] = tg[pl.ds(c, jg, stride=chans), :].astype(bf16)

        def body(t, carry):
            table = tx[1 - f, pl.ds(pl.multiple_of(t * 2 * LANES, LANES), 2 * LANES), :]
            r = dot_t(lhs2[...], table, 1, 1).astype(bf16)
            for h in range(2):
                isb[f, p, t * 2 + h] = r[:, h * LANES:(h + 1) * LANES].reshape(groups, jg, LANES)
            return carry

        lax.fori_loop(0, nx // 2, body, 0, unroll=2)
        into = back_ref if f else gbuf
        into[p, :, jrows(gx), :] = isb[f, p, gx]
        for o in range(1, nx):
            back(f, p, o, True).start()

    def open_point(p):
        load_cot(p).wait()
        for o in range(1, nx):
            back(0, p, o, False).wait_recv()

        def turn(g, carry):
            block = gbuf[p, g].T.reshape(per, halves, PACK, modes)
            for h in range(halves):
                gt[h, pl.ds(g * per * PACK, per * PACK), :] = block[:, h].reshape(per * PACK, modes)
            return carry

        lax.fori_loop(0, groups, turn, 0, unroll=4)

    def pieces(lo, hi, p):
        def piece(s, carry):
            h, y = s // parts, s % parts
            rows16 = pl.ds(pl.multiple_of(h * PACK, PACK), PACK)
            cols = pl.ds(pl.multiple_of(y * width, width), width)
            xs[...] = fbuf[p, :, rows16, cols].reshape(chans * PACK, width)
            r = jnp.dot(kron[...], xs[...], preferred_element_type=f32)
            r = r + jnp.dot(gt[h], iy_ref[:, cols], preferred_element_type=f32)
            pre[...] = r.reshape(chans, PACK, width)

            def one(c, inner):
                v = pre[c] + bias_ref[c]
                phi = 0.5 + 0.5 * lax.erf(v * root_half)
                density = jnp.exp(-0.5 * v * v) * density_norm
                cot = cbuf[p, c, rows16, cols].astype(f32)
                cbuf[p, c, rows16, cols] = (v * phi).astype(bf16)
                fbuf[p, c, rows16, cols] = (cot * (phi + v * density)).astype(bf16)
                return inner

            lax.fori_loop(0, chans, one, 0, unroll=8)
            return carry

        lax.fori_loop(lo, hi, piece, 0)

    total = halves * parts

    def point_part(i, p):
        if i == 0:
            open_point(p)
        pieces(i * total // 2, (i + 1) * total // 2, p)

    def turn_home(p):
        analyse(1, p)
        send_rows(1, p)

    def through(p):
        def piece(s, carry):
            h, y = s // parts, s % parts
            rows16 = pl.ds(pl.multiple_of(h * PACK, PACK), PACK)
            cols = pl.ds(pl.multiple_of(y * width, width), width)
            xs[...] = fbuf[p, :, rows16, cols].reshape(chans * PACK, width)
            r = jnp.dot(kron_t[...], xs[...], preferred_element_type=f32)
            fbuf[p, :, rows16, cols] = r.astype(bf16).reshape(chans, PACK, width)
            return carry

        lax.fori_loop(0, halves * parts, piece, 0)

    load(0).wait()
    analyse(0, 0)
    pl.semaphore_wait(barrier, nx + ny - 2)
    send_rows(0, 0)

    def first(p, carry):
        load(p).wait()
        analyse(0, p)
        send_rows(0, p)
        return carry

    lax.fori_loop(1, planes, first, 0)

    tx[...] = jnp.zeros_like(tx)
    for f, ref in enumerate((fx_ref, ix_ref)):
        for s in range(nx):
            for c in range(per):
                tx[f, pl.ds(s * LANES + c * slab, slab), pl.ds(c * modes, modes)] = ref[s, gy]

    tall = chans * PACK
    row = lax.broadcasted_iota(jnp.int32, (tall, chans), 0) // PACK
    col = lax.broadcasted_iota(jnp.int32, (tall, chans), 1)
    pick = jnp.where(row == col, 1.0, 0.0).astype(bf16)
    right = dot_t(lw_ref[...], pick, 1, 1).astype(bf16)
    left = dot_t(lw_ref[...], pick, 0, 1).astype(bf16)
    cut = 2 * LANES
    for k in range(tall // cut):
        sub = pick[k * cut:(k + 1) * cut]
        keep = (lax.broadcasted_iota(jnp.int32, (cut, tall), 0) % PACK
                == lax.broadcasted_iota(jnp.int32, (cut, tall), 1) % PACK)
        rows_k = pl.ds(k * cut, cut)
        kron_t[rows_k, :] = jnp.where(keep, jnp.dot(sub, right, preferred_element_type=f32), 0.0).astype(bf16)
        kron[rows_k, :] = jnp.where(keep, jnp.dot(sub, left, preferred_element_type=f32), 0.0).astype(bf16)
    load_w().wait()

    def step(t, carry):
        def stage(lag, run):
            @pl.when((t >= lag) & (t < planes + lag))
            def _():
                run(t - lag)

        for lag, run in plan:
            stage(lag, run)
        return carry

    forth = lambda fn: functools.partial(fn, 0)
    home = lambda fn: functools.partial(fn, 1)
    half = lambda i: functools.partial(point_part, i)
    plan = (
        (0, forth(across)),
        (6, home(across)),
        (8, home(relay_mixed)),
        (7, home(mix)),
        (10, through),
        (1, forth(relay_sums)),
        (3, forth(expand)),
        (4, half(0)),
        (6, home(relay_sums)),
        (2, forth(relay_mixed)),
        (4, half(1)),
        (4, turn_home),
        (8, home(expand)),
        (1, forth(mix)),
    )

    lax.fori_loop(0, planes + max(lag for lag, _ in plan), step, 0)

    def finish(p, carry):
        for f in range(2):
            for o in range(1, nx):
                rows(f, p, o, True).wait_send()
                back(f, p, o, True).wait_send()
            gy_sent(f, p)
        for o in range(1, nx):
            back(1, p, o, False).wait_recv()
        return carry

    lax.fori_loop(0, planes, finish, 0)


def main_pass(nx, ny, flow, cot, weight, local_weight, bias, fwd_y, inv_y, fwd_x, inv_x):
    planes, chans, slab, cells = flow.shape
    own, modes = weight.shape[0], weight.shape[3]
    per = LANES // slab
    groups = chans // per
    jg = modes // nx
    tall = chans * PACK
    vm = pl.BlockSpec(memory_space=pltpu.VMEM)
    hbm = pl.BlockSpec(memory_space=pl.ANY)
    dma = pltpu.SemaphoreType.DMA
    split = lambda t: t.reshape(nx, ny, slab, modes)
    field = pltpu.VMEM(flow.shape, bf16)
    coef = pltpu.VMEM((planes, own, chans, modes), bf16)
    return pl.pallas_call(
        functools.partial(main_kernel, nx, ny, planes, chans, slab, modes, own),
        out_shape=(
            field, field,
            pltpu.VMEM((planes, groups, modes, LANES), bf16),
            coef, coef,
        ),
        in_specs=[hbm, hbm, hbm, vm, pl.BlockSpec(memory_space=pltpu.SMEM), vm, vm, vm, vm],
        out_specs=(vm, vm, vm, vm, vm),
        scratch_shapes=[
            pltpu.VMEM(weight.shape, bf16),
            pltpu.VMEM((2, nx * LANES, per * modes), bf16),
            pltpu.VMEM((tall, tall), bf16),
            pltpu.VMEM((tall, tall), bf16),
            pltpu.VMEM((2, planes, nx, groups, jg, LANES), bf16),
            pltpu.VMEM((2, planes, groups, jg, nx * LANES), bf16),
            pltpu.VMEM((chans * jg, modes), f32),
            pltpu.VMEM((2, planes, ny, own, chans, modes), bf16),
            pltpu.VMEM((2, planes, ny, own, chans, modes), bf16),
            pltpu.VMEM((2, planes, 2, own, chans, modes), bf16),
            pltpu.VMEM((own * chans, modes), f32),
            pltpu.VMEM((2, planes, own, chans, modes), bf16),
            pltpu.VMEM((2, planes, ny, own, chans, modes), bf16),
            pltpu.VMEM((ny * own * chans, modes), f32),
            pltpu.VMEM((groups * jg, per * modes), bf16),
            pltpu.VMEM((2, planes, nx, groups, jg, LANES), bf16),
            pltpu.VMEM((planes, groups, modes, LANES), bf16),
            pltpu.VMEM((slab // PACK, tall, modes), bf16),
            pltpu.VMEM((chans, PACK, 2 * LANES), f32),
            pltpu.VMEM((tall, 2 * LANES), bf16),
            dma((planes,)), dma((planes,)), dma,
            dma((2, planes, nx)), dma((2, planes, nx)),
            dma((2, planes, ny)), dma((2, planes, ny)),
            dma((2, planes, ny)), dma((2, planes, ny)),
            dma((2, planes, nx)), dma((2, planes, nx)),
        ],
        compiler_params=pltpu.CompilerParams(
            collective_id=0, has_side_effects=True, vmem_limit_bytes=40 << 20),
        name="main_pass",
    )(flow, cot, weight, local_weight, bias, fwd_y.T, inv_y.T, split(fwd_x), split(inv_x))


def rows_by_half(g_ref, p, gt):
    groups = g_ref.shape[1]
    halves, tall, modes = gt.shape
    slab = halves * PACK
    per = LANES // slab

    def turn(g, carry):
        block = g_ref[p, g].T.reshape(per, halves, PACK, modes)
        for h in range(halves):
            gt[h, pl.ds(g * per * PACK, per * PACK), :] = block[:, h].reshape(per * PACK, modes)
        return carry

    lax.fori_loop(0, groups, turn, 0, unroll=4)


def last_kernel(thru_ref, g_ref, yt_ref, co_ref, gm_ref, held_ref, out_ref, gs_ref, keep_hbm, gt, cf, sem):
    _, chans, slab, width = out_ref.shape
    planes, own = co_ref.shape[:2]
    rows_here = gs_ref.shape[0]
    p, part = pl.program_id(0), pl.program_id(1)

    def keep(q):
        return pltpu.make_async_copy(held_ref.at[q], keep_hbm.at[q], sem.at[q])

    @pl.when(part == 0)
    def _():
        keep(p).start()
        rows_by_half(g_ref, p, gt)

    cols = pl.ds(pl.multiple_of(part * width, width), width)
    for h in range(slab // PACK):
        r = jnp.dot(gt[h], yt_ref[...], preferred_element_type=f32).reshape(chans, PACK, width)
        r = r + thru_ref[p, :, h * PACK:(h + 1) * PACK, cols].astype(f32)
        out_ref[0, :, h * PACK:(h + 1) * PACK, :] = r.astype(bf16)

    first = (p * pl.num_programs(1) + part) * rows_here
    j, i = first // chans, pl.multiple_of(first % chans, rows_here)
    cf[...] = co_ref[:, j, pl.ds(i, rows_here), :].astype(f32).reshape(cf.shape)

    def outer(r, carry):
        total = cf[pl.ds(r, 1), :] * gm_ref[0, j].astype(f32)
        for q in range(1, planes):
            total = total + cf[pl.ds(q * rows_here + r, 1), :] * gm_ref[q, j].astype(f32)
        gs_ref[r] = total
        return carry

    lax.fori_loop(0, rows_here, outer, 0, unroll=4)

    @pl.when((p == planes - 1) & (part == pl.num_programs(1) - 1))
    def _():
        for q in range(planes):
            keep(q).wait()


def last_pass(thru, g, table_y, co, gm, held, parts):
    planes, chans, slab, cells = thru.shape
    modes, own = g.shape[2], co.shape[1]
    width = cells // parts
    rows_here = own * chans // (planes * parts)
    field = pl.BlockSpec((1, chans, slab, width), lambda p, h: (p, 0, 0, h))
    whole = pl.BlockSpec(memory_space=pltpu.VMEM)
    shape = jax.ShapeDtypeStruct(thru.shape, bf16)
    return pl.pallas_call(
        last_kernel,
        grid=(planes, parts),
        out_shape=(shape, jax.ShapeDtypeStruct((own * chans, chans, modes), f32), shape),
        in_specs=[
            whole,
            whole,
            pl.BlockSpec((modes, width), lambda p, h: (0, h)),
            whole, whole, whole,
        ],
        out_specs=(
            field,
            pl.BlockSpec((rows_here, chans, modes), lambda p, h: (p * parts + h, 0, 0)),
            pl.BlockSpec(memory_space=pl.ANY),
        ),
        scratch_shapes=[
            pltpu.VMEM((slab // PACK, chans * PACK, modes), bf16),
            pltpu.VMEM((planes * rows_here, modes), f32),
            pltpu.SemaphoreType.DMA((planes,)),
        ],
        compiler_params=pltpu.CompilerParams(vmem_limit_bytes=20 << 20),
        name="last_pass",
    )(thru, g, table_y.T, co, gm, held)


def kernel_shards(nx, ny, flow_field, cotangent, spectral_weight, local_weight, channel_bias):
    planes, chans, slab, cells = flow_field.shape
    across = slab * nx * ny
    own, modes = spectral_weight.shape[0], spectral_weight.shape[3]
    scale_inv = math.sqrt(1.0 / (modes // 2))
    fwd_x = basis_table(across, modes, math.sqrt(2.0 / across))
    fwd_y = basis_table(cells, modes, math.sqrt(2.0 / cells))
    inv_x = basis_table(across, modes, scale_inv)
    inv_y = basis_table(cells, modes, scale_inv)
    out, thru, back, coeffs, grad_mixed = main_pass(
        nx, ny, flow_field, cotangent, spectral_weight, local_weight, channel_bias, fwd_y, inv_y, fwd_x, inv_x)
    grad_field, grad_spectral, out = last_pass(thru, back, fwd_y, coeffs, grad_mixed, out, 2)
    return out, grad_field, grad_spectral.reshape(own, chans, chans, modes)


def solution(mesh):
    nx, ny = mesh.shape["gx"], mesh.shape["gy"]

    def shards(flow_field, cotangent, spectral_weight, local_weight, channel_bias):
        planes, chans, slab, cells = flow_field.shape
        own, modes = spectral_weight.shape[0], spectral_weight.shape[3]
        fits = (
            slab % PACK == 0 and LANES % slab == 0 and modes == LANES
            and nx % 2 == 0 and ny == 4 and (modes // nx) % PACK == 0
            and chans % (2 * LANES // slab) == 0 and chans % PACK == 0
            and cells % (2 * LANES) == 0
            and own * nx * ny == modes and chans % (own * chans // (2 * planes)) == 0
        )
        args = (flow_field, cotangent, spectral_weight, local_weight, channel_bias)
        return kernel_shards(nx, ny, *args) if fits else plain_shards(*args)

    placed = (
        P(None, None, ("gx", "gy"), None),
        P(None, None, ("gx", "gy"), None),
        P(("gx", "gy"), None, None, None),
        P(),
        P(),
    )
    return jax.shard_map(
        shards,
        mesh=mesh,
        in_specs=placed,
        out_specs=(
            P(None, None, ("gx", "gy"), None),
            P(None, None, ("gx", "gy"), None),
            P(("gx", "gy"), None, None, None),
        ),
        check_vma=False,
    )
```

```python
import functools
import math

import jax
import jax.numpy as jnp
import numpy as np
from jax import lax
from jax.experimental import pallas as pl
from jax.experimental.pallas import tpu as pltpu
from jax.sharding import PartitionSpec as P

root_half = 0.7071067811865476
density_norm = 0.3989422804014327
LANES = 128
PACK = 16
MESH = pl.DeviceIdType.MESH
f32, bf16 = jnp.float32, jnp.bfloat16


def basis_table(cells, cols, factor):
    kept = cols // 2
    columns = np.arange(cols)
    frequency = np.where(columns < kept, columns, columns - kept + 1)
    phases = np.arange(cells)[:, None] * frequency[None, :] % cells
    angles = phases.astype(np.float32) * np.float32(2.0 * math.pi / cells)
    values = np.where(columns[None, :] < kept, np.cos(angles), np.sin(angles))
    return jnp.asarray((values * np.float32(factor)).astype(jnp.bfloat16))


def gelu_slope(values):
    cumulative = 0.5 * (1.0 + lax.erf(values * root_half))
    density = jnp.exp(-0.5 * values * values) * density_norm
    return cumulative + values * density


def dot_t(a, b, da, db):
    return lax.dot_general(a, b, (((da,), (db,)), ((), ())), preferred_element_type=f32)


def to_owners(modal_rows):
    return lax.all_to_all(modal_rows, ("gx", "gy"), split_axis=0, concat_axis=1, tiled=True)


def to_slabs(modal_part):
    return lax.all_to_all(modal_part, ("gx", "gy"), split_axis=1, concat_axis=0, tiled=True)


def contract(spec, left, right):
    return jnp.einsum(spec, left, right, preferred_element_type=jnp.float32)


def plain_shards(flow_field, cotangent, spectral_weight, local_weight, channel_bias):
    devices = lax.axis_size("gx") * lax.axis_size("gy")
    planes, channels, slab_rows, cells_along = flow_field.shape
    cells_across = slab_rows * devices
    own_cols = spectral_weight.shape[0]
    mode_cols = spectral_weight.shape[3]
    kept_modes = mode_cols // 2
    both = planes * channels
    scale_inv = math.sqrt(1.0 / kept_modes)
    fwd_x = basis_table(cells_across, mode_cols, math.sqrt(2.0 / cells_across))
    fwd_y = basis_table(cells_along, mode_cols, math.sqrt(2.0 / cells_along))
    inv_x = basis_table(cells_across, mode_cols, scale_inv)
    inv_y = basis_table(cells_along, mode_cols, scale_inv)

    def to_modes(field, table_x, table_y):
        rows = contract("axy,yj->jxa", field.reshape(both, slab_rows, cells_along), table_y)
        received = to_owners(rows.astype(jnp.bfloat16))
        modes = contract("jxa,xk->jka", received, table_x).astype(jnp.bfloat16)
        return modes.reshape(own_cols, mode_cols, planes, channels)

    def to_rows(modes, table_x):
        merged = modes.reshape(own_cols, mode_cols, both)
        return to_slabs(contract("jka,xk->jxa", merged, table_x).astype(jnp.bfloat16))

    def to_space(rows, table_y):
        field = contract("jxa,yj->axy", rows, table_y)
        return field.reshape(planes, channels, slab_rows, cells_along)

    coeffs = to_modes(flow_field, fwd_x, fwd_y)
    mixed = contract("jkzi,jiok->jkzo", coeffs, spectral_weight).astype(jnp.bfloat16)
    gathered = to_rows(mixed, inv_x)
    spectral = to_space(gathered, inv_y)
    pointwise = contract("zixy,io->zoxy", flow_field, local_weight)
    pre_activation = spectral + pointwise + channel_bias[None, :, None, None]
    output_field = jax.nn.gelu(pre_activation, approximate=False).astype(jnp.bfloat16)
    grad_pre = (cotangent.astype(jnp.float32) * gelu_slope(pre_activation)).astype(jnp.bfloat16)
    grad_mixed = to_modes(grad_pre, inv_x, inv_y)
    grad_coeffs = contract("jkzo,jiok->jkzi", grad_mixed, spectral_weight).astype(jnp.bfloat16)
    gathered_back = to_rows(grad_coeffs, fwd_x)
    grad_spectral = contract("jkzi,jkzo->jiok", coeffs, grad_mixed)
    backward = to_space(gathered_back, fwd_y)
    through_local = contract("zoxy,io->zixy", grad_pre, local_weight)
    grad_field = (backward + through_local).astype(jnp.bfloat16)
    return (output_field, grad_field, grad_spectral)


def main_kernel(
    nx, ny, planes, chans, slab, modes, own,
    flow_hbm, cot_hbm, w_hbm, lw_ref, bias_ref, fy_ref, iy_ref, fx_ref, ix_ref,
    cbuf, fbuf, back_ref, co_ref, gm_ref,
    wbuf, tx, kron, kron_t, sbuf, rbuf, part, zs, zr, zq, cf, ms, zg, tg, lhs2, isb,
    gbuf, gt, pre, xs,
    load_sem, cot_sem, w_sem, s1, r1, s2, r2, s3, r3, s4, r4,
):
    gx, gy = lax.axis_index("gx"), lax.axis_index("gy")
    per = LANES // slab
    groups = chans // per
    jg = modes // nx
    cells = fbuf.shape[3]
    halves = slab // PACK
    width = 2 * LANES
    parts = cells // width

    def load(p):
        return pltpu.make_async_copy(flow_hbm.at[p], fbuf.at[p], load_sem.at[p])

    def load_cot(p):
        return pltpu.make_async_copy(cot_hbm.at[p], cbuf.at[p], cot_sem.at[p])

    def load_w():
        return pltpu.make_async_copy(w_hbm, wbuf, w_sem)

    for p in range(planes):
        load(p).start()
    load_w().start()
    for p in range(planes):
        load_cot(p).start()

    barrier = pltpu.get_barrier_semaphore()
    for o in range(1, nx):
        pl.semaphore_signal(barrier, inc=1, device_id=((gx + o) % nx, gy), device_id_type=MESH)
    for o in range(1, ny):
        pl.semaphore_signal(barrier, inc=1, device_id=(gx, (gy + o) % ny), device_id_type=MESH)

    def lane(g):
        return pl.ds(pl.multiple_of(g * LANES, LANES), LANES)

    def jrows(g):
        return pl.ds(pl.multiple_of(g * jg, jg), jg)

    def rows(f, p, o, out):
        other = (gx + o) % nx if out else (gx + nx - o) % nx
        slot = gx if out else other
        return pltpu.make_async_remote_copy(
            sbuf.at[f, p, other], rbuf.at[f, p, :, :, lane(slot)], s1.at[f, p, o], r1.at[f, p, o],
            device_id=(other, gy), device_id_type=MESH)

    side = gy // 2
    outer, inner = 3 * side, 1 + side
    far_inner, far_outer = 2 - side, 3 - 3 * side
    partner = outer + inner - gy
    at_inner = gy == inner
    at_outer = gy != inner

    def along(f, p, src, dst, to, sent, got):
        return pltpu.make_async_remote_copy(
            src, dst, sent, got, device_id=(gx, to), device_id_type=MESH)

    def sums_near(f, p, i, dest, to):
        return along(f, p, zs.at[f, p, dest], zr.at[f, p, i], to, s2.at[f, p, i], r2.at[f, p, i])

    def sums_far(f, p, i, to):
        return along(f, p, zq.at[f, p, i], zr.at[f, p, 3], to, s2.at[f, p, 1 + i], r2.at[f, p, 3])

    def mixed_near(f, p, i, slot, to):
        return along(f, p, ms.at[f, p], zg.at[f, p, slot], to, s3.at[f, p, i], r3.at[f, p, slot])

    def mixed_on(f, p, i, slot, to):
        return along(f, p, zg.at[f, p, slot], zg.at[f, p, slot], to, s3.at[f, p, 2 + i], r3.at[f, p, slot])

    def send_sums(f, p):
        @pl.when(at_outer)
        def _():
            for i, dest in ((2, far_outer), (1, far_inner), (0, inner)):
                sums_near(f, p, i, dest, inner).start()

        @pl.when(at_inner)
        def _():
            sums_near(f, p, 0, outer, outer).start()

    def relay_sums(f, p):
        @pl.when(at_inner)
        def _():
            for i, dest in ((1, far_outer), (0, far_inner)):
                sums_near(f, p, 1 + i, gy, outer).wait_recv()
                zq[f, p, i] = (zr[f, p, 1 + i].astype(f32) + zs[f, p, dest].astype(f32)).astype(bf16)
                sums_far(f, p, i, dest).start()

    def take_sums(f, p):
        sums_near(f, p, 0, gy, partner).wait_recv()
        sums_far(f, p, 0, far_inner).wait_recv()
        return zs[f, p, gy].astype(f32) + zr[f, p, 0].astype(f32) + zr[f, p, 3].astype(f32)

    def send_mixed(f, p):
        mixed_near(f, p, 1, gy, far_inner).start()
        mixed_near(f, p, 0, gy, partner).start()

    def relay_mixed(f, p):
        @pl.when(at_inner)
        def _():
            for i, slot in enumerate((far_inner, far_outer)):
                mixed_near(f, p, i, slot, slot).wait_recv()
                mixed_on(f, p, i, slot, outer).start()

    def take_mixed(f, p):
        mixed_near(f, p, 0, partner, partner).wait_recv()

        @pl.when(at_outer)
        def _():
            for i, slot in enumerate((far_inner, far_outer)):
                mixed_on(f, p, i, slot, inner).wait_recv()

    def gy_sent(f, p):
        @pl.when(at_outer)
        def _():
            for i, dest in enumerate((inner, far_inner, far_outer)):
                sums_near(f, p, i, dest, inner).wait_send()

        @pl.when(at_inner)
        def _():
            sums_near(f, p, 0, outer, outer).wait_send()
            for i, dest in enumerate((far_inner, far_outer)):
                sums_far(f, p, i, dest).wait_send()
                mixed_on(f, p, i, dest, outer).wait_send()

        mixed_near(f, p, 0, gy, partner).wait_send()
        mixed_near(f, p, 1, gy, far_inner).wait_send()

    def back(f, p, o, out):
        other = (gx + o) % nx if out else (gx + nx - o) % nx
        slot = gx if out else other
        into = back_ref if f else gbuf
        return pltpu.make_async_remote_copy(
            isb.at[f, p, other], into.at[p, :, jrows(slot), :], s4.at[f, p, o], r4.at[f, p, o],
            device_id=(other, gy), device_id_type=MESH)

    def analyse(f, p):
        table = iy_ref if f else fy_ref

        wide = groups // 2

        def body(t, carry):
            x = fbuf[p, pl.ds(t * wide * per, wide * per)].reshape(wide * LANES, cells)
            r = dot_t(table[...], x, 1, 1).astype(bf16)
            for h in range(wide):
                sbuf[f, p, :, t * wide + h] = r[:, h * LANES:(h + 1) * LANES].reshape(nx, jg, LANES)
            return carry

        lax.fori_loop(0, 2, body, 0)
        rbuf[f, p, :, :, lane(gx)] = sbuf[f, p, gx]

    def send_rows(f, p):
        for o in range(1, nx):
            rows(f, p, o, True).start()

    def across(f, p):
        for o in range(1, nx):
            rows(f, p, o, False).wait_recv()
        left = rbuf[f, p].reshape(groups * jg, nx * LANES)
        r = jnp.dot(left, tx[f], preferred_element_type=f32)
        for g in range(groups):
            for c in range(per):
                part[pl.ds((g * per + c) * jg, jg), :] = r[g * jg:(g + 1) * jg, c * modes:(c + 1) * modes]
        for j in range(jg):
            zs[f, p, j // own, j % own] = part[pl.ds(j, chans, stride=jg), :].astype(bf16)
        send_sums(f, p)

    def mix(f, p):
        coef = take_sums(f, p).astype(bf16)
        if f:
            gm_ref[p] = coef
        else:
            co_ref[p] = coef
        cf[...] = coef.astype(f32).reshape(own * chans, modes)
        for j in range(own):
            if f:
                right = cf[pl.ds(j * chans, chans), :]

                def body(i, carry):
                    prod = wbuf[j, i].astype(f32) * right
                    part[pl.ds(pl.multiple_of(i * 8, 8), 8), :] = jnp.sum(prod.reshape(chans // 8, 8, modes), axis=0)
                    return carry

                lax.fori_loop(0, chans, body, 0, unroll=8)
                total = part[pl.ds(0, chans, stride=8), :]
                for k in range(1, 8):
                    total = total + part[pl.ds(k, chans, stride=8), :]
                ms[f, p, j] = total.astype(bf16)
            else:

                def body(i, acc):
                    return acc + cf[pl.ds(j * chans + i, 1), :] * wbuf[j, i].astype(f32)

                acc = lax.fori_loop(0, chans, body, jnp.zeros((chans, modes), f32), unroll=8)
                ms[f, p, j] = acc.astype(bf16)
        zg[f, p, gy] = ms[f, p]
        send_mixed(f, p)

    def expand(f, p):
        take_mixed(f, p)
        tg[...] = zg[f, p].astype(f32).reshape(ny * own * chans, modes)
        for c in range(chans):
            lhs2[pl.ds((c // per) * jg, jg), pl.ds((c % per) * modes, modes)] = tg[pl.ds(c, jg, stride=chans), :].astype(bf16)

        def body(t, carry):
            table = tx[1 - f, pl.ds(pl.multiple_of(t * 2 * LANES, LANES), 2 * LANES), :]
            r = dot_t(lhs2[...], table, 1, 1).astype(bf16)
            for h in range(2):
                isb[f, p, t * 2 + h] = r[:, h * LANES:(h + 1) * LANES].reshape(groups, jg, LANES)
            return carry

        lax.fori_loop(0, nx // 2, body, 0, unroll=2)
        into = back_ref if f else gbuf
        into[p, :, jrows(gx), :] = isb[f, p, gx]
        for o in range(1, nx):
            back(f, p, o, True).start()

    def open_point(p):
        load_cot(p).wait()
        for o in range(1, nx):
            back(0, p, o, False).wait_recv()

        def turn(g, carry):
            block = gbuf[p, g].T.reshape(per, halves, PACK, modes)
            for h in range(halves):
                gt[h, pl.ds(g * per * PACK, per * PACK), :] = block[:, h].reshape(per * PACK, modes)
            return carry

        lax.fori_loop(0, groups, turn, 0, unroll=4)

    def pieces(lo, hi, p):
        def place(s):
            h, y = s // parts, s % parts
            return h, pl.ds(h * PACK, PACK), pl.ds(y * width, width)

        def product(s, into):
            h, rows16, cols = place(s)
            xs[s % 2] = fbuf[p, :, rows16, cols].reshape(chans * PACK, width)
            r = jnp.dot(kron[...], xs[s % 2], preferred_element_type=f32)
            r = r + jnp.dot(gt[h], iy_ref[:, cols], preferred_element_type=f32)
            into[...] = r.reshape(chans, PACK, width)

        def one(s, held, c):
            _, rows16, cols = place(s)
            v = held[c] + bias_ref[c]
            phi = 0.5 + 0.5 * lax.erf(v * root_half)
            density = jnp.exp(-0.5 * v * v) * density_norm
            cot = cbuf[p, c, rows16, cols].astype(f32)
            cbuf[p, c, rows16, cols] = (v * phi).astype(bf16)
            fbuf[p, c, rows16, cols] = (cot * (phi + v * density)).astype(bf16)

        def rest(s, held):
            def body(c, carry):
                one(s, held, c)
                return carry

            lax.fori_loop(0, chans, body, 0, unroll=8)

        product(lo, pre.at[0])
        for s in range(lo + 1, hi):
            product(s, pre.at[s - lo])
            for c in range(chans):
                one(s - 1, pre.at[s - 1 - lo], c)
        rest(hi - 1, pre.at[hi - 1 - lo])

    total = halves * parts

    def point_part(i, p):
        if i == 0:
            open_point(p)
        pieces(i * total // 2, (i + 1) * total // 2, p)

    def turn_home(p):
        analyse(1, p)
        send_rows(1, p)

    def through(p):
        def piece(s, carry):
            h, y = s // parts, s % parts
            rows16 = pl.ds(pl.multiple_of(h * PACK, PACK), PACK)
            cols = pl.ds(pl.multiple_of(y * width, width), width)
            xs[0] = fbuf[p, :, rows16, cols].reshape(chans * PACK, width)
            r = jnp.dot(kron_t[...], xs[0], preferred_element_type=f32)
            fbuf[p, :, rows16, cols] = r.astype(bf16).reshape(chans, PACK, width)
            return carry

        lax.fori_loop(0, halves * parts, piece, 0)

    load(0).wait()
    analyse(0, 0)
    pl.semaphore_wait(barrier, nx + ny - 2)
    send_rows(0, 0)

    def first(p, carry):
        load(p).wait()
        analyse(0, p)
        send_rows(0, p)
        return carry

    lax.fori_loop(1, planes, first, 0)

    tx[...] = jnp.zeros_like(tx)
    for f, ref in enumerate((fx_ref, ix_ref)):
        for s in range(nx):
            for c in range(per):
                tx[f, pl.ds(s * LANES + c * slab, slab), pl.ds(c * modes, modes)] = ref[s, gy]

    tall = chans * PACK
    row = lax.broadcasted_iota(jnp.int32, (tall, chans), 0) // PACK
    col = lax.broadcasted_iota(jnp.int32, (tall, chans), 1)
    pick = jnp.where(row == col, 1.0, 0.0).astype(bf16)
    right = dot_t(lw_ref[...], pick, 1, 1).astype(bf16)
    left = dot_t(lw_ref[...], pick, 0, 1).astype(bf16)
    cut = 2 * LANES
    for k in range(tall // cut):
        sub = pick[k * cut:(k + 1) * cut]
        keep = (lax.broadcasted_iota(jnp.int32, (cut, tall), 0) % PACK
                == lax.broadcasted_iota(jnp.int32, (cut, tall), 1) % PACK)
        rows_k = pl.ds(k * cut, cut)
        kron_t[rows_k, :] = jnp.where(keep, jnp.dot(sub, right, preferred_element_type=f32), 0.0).astype(bf16)
        kron[rows_k, :] = jnp.where(keep, jnp.dot(sub, left, preferred_element_type=f32), 0.0).astype(bf16)
    load_w().wait()

    def step(t, carry):
        def stage(lag, run):
            @pl.when((t >= lag) & (t < planes + lag))
            def _():
                run(t - lag)

        for lag, run in plan:
            stage(lag, run)
        return carry

    forth = lambda fn: functools.partial(fn, 0)
    home = lambda fn: functools.partial(fn, 1)
    half = lambda i: functools.partial(point_part, i)
    plan = (
        (6, home(across)),
        (8, home(relay_mixed)),
        (7, home(mix)),
        (0, forth(across)),
        (10, through),
        (1, forth(relay_sums)),
        (3, forth(expand)),
        (4, half(0)),
        (6, home(relay_sums)),
        (2, forth(relay_mixed)),
        (4, half(1)),
        (4, turn_home),
        (8, home(expand)),
        (1, forth(mix)),
    )

    lax.fori_loop(0, planes + max(lag for lag, _ in plan), step, 0)

    def finish(p, carry):
        for f in range(2):
            for o in range(1, nx):
                rows(f, p, o, True).wait_send()
                back(f, p, o, True).wait_send()
            gy_sent(f, p)
        for o in range(1, nx):
            back(1, p, o, False).wait_recv()
        return carry

    lax.fori_loop(0, planes, finish, 0)


def main_pass(nx, ny, flow, cot, weight, local_weight, bias, fwd_y, inv_y, fwd_x, inv_x):
    planes, chans, slab, cells = flow.shape
    own, modes = weight.shape[0], weight.shape[3]
    per = LANES // slab
    groups = chans // per
    jg = modes // nx
    tall = chans * PACK
    vm = pl.BlockSpec(memory_space=pltpu.VMEM)
    hbm = pl.BlockSpec(memory_space=pl.ANY)
    dma = pltpu.SemaphoreType.DMA
    split = lambda t: t.reshape(nx, ny, slab, modes)
    field = pltpu.VMEM(flow.shape, bf16)
    coef = pltpu.VMEM((planes, own, chans, modes), bf16)
    return pl.pallas_call(
        functools.partial(main_kernel, nx, ny, planes, chans, slab, modes, own),
        out_shape=(
            field, field,
            pltpu.VMEM((planes, groups, modes, LANES), bf16),
            coef, coef,
        ),
        in_specs=[hbm, hbm, hbm, vm, pl.BlockSpec(memory_space=pltpu.SMEM), vm, vm, vm, vm],
        out_specs=(vm, vm, vm, vm, vm),
        scratch_shapes=[
            pltpu.VMEM(weight.shape, bf16),
            pltpu.VMEM((2, nx * LANES, per * modes), bf16),
            pltpu.VMEM((tall, tall), bf16),
            pltpu.VMEM((tall, tall), bf16),
            pltpu.VMEM((2, planes, nx, groups, jg, LANES), bf16),
            pltpu.VMEM((2, planes, groups, jg, nx * LANES), bf16),
            pltpu.VMEM((chans * jg, modes), f32),
            pltpu.VMEM((2, planes, ny, own, chans, modes), bf16),
            pltpu.VMEM((2, planes, ny, own, chans, modes), bf16),
            pltpu.VMEM((2, planes, 2, own, chans, modes), bf16),
            pltpu.VMEM((own * chans, modes), f32),
            pltpu.VMEM((2, planes, own, chans, modes), bf16),
            pltpu.VMEM((2, planes, ny, own, chans, modes), bf16),
            pltpu.VMEM((ny * own * chans, modes), f32),
            pltpu.VMEM((groups * jg, per * modes), bf16),
            pltpu.VMEM((2, planes, nx, groups, jg, LANES), bf16),
            pltpu.VMEM((planes, groups, modes, LANES), bf16),
            pltpu.VMEM((slab // PACK, tall, modes), bf16),
            pltpu.VMEM((2, chans, PACK, 2 * LANES), f32),
            pltpu.VMEM((2, tall, 2 * LANES), bf16),
            dma((planes,)), dma((planes,)), dma,
            dma((2, planes, nx)), dma((2, planes, nx)),
            dma((2, planes, ny)), dma((2, planes, ny)),
            dma((2, planes, ny)), dma((2, planes, ny)),
            dma((2, planes, nx)), dma((2, planes, nx)),
        ],
        compiler_params=pltpu.CompilerParams(
            collective_id=0, has_side_effects=True, vmem_limit_bytes=40 << 20),
        name="main_pass",
    )(flow, cot, weight, local_weight, bias, fwd_y.T, inv_y.T, split(fwd_x), split(inv_x))


def rows_by_half(g_ref, p, gt):
    groups = g_ref.shape[1]
    halves, tall, modes = gt.shape
    slab = halves * PACK
    per = LANES // slab

    def turn(g, carry):
        block = g_ref[p, g].T.reshape(per, halves, PACK, modes)
        for h in range(halves):
            gt[h, pl.ds(g * per * PACK, per * PACK), :] = block[:, h].reshape(per * PACK, modes)
        return carry

    lax.fori_loop(0, groups, turn, 0, unroll=4)


def last_kernel(thru_ref, g_ref, yt_ref, co_ref, gm_ref, held_ref, out_ref, gs_ref, keep_hbm, gt, cf, sem):
    _, chans, slab, width = out_ref.shape
    planes, own = co_ref.shape[:2]
    rows_here = gs_ref.shape[0]
    p, part = pl.program_id(0), pl.program_id(1)

    def keep(q):
        return pltpu.make_async_copy(held_ref.at[q], keep_hbm.at[q], sem.at[q])

    @pl.when(part == 0)
    def _():
        keep(p).start()
        rows_by_half(g_ref, p, gt)

    cols = pl.ds(pl.multiple_of(part * width, width), width)
    for h in range(slab // PACK):
        r = jnp.dot(gt[h], yt_ref[...], preferred_element_type=f32).reshape(chans, PACK, width)
        r = r + thru_ref[p, :, h * PACK:(h + 1) * PACK, cols].astype(f32)
        out_ref[0, :, h * PACK:(h + 1) * PACK, :] = r.astype(bf16)

    first = (p * pl.num_programs(1) + part) * rows_here
    j, i = first // chans, pl.multiple_of(first % chans, rows_here)
    cf[...] = co_ref[:, j, pl.ds(i, rows_here), :].astype(f32).reshape(cf.shape)

    def outer(r, carry):
        total = cf[pl.ds(r, 1), :] * gm_ref[0, j].astype(f32)
        for q in range(1, planes):
            total = total + cf[pl.ds(q * rows_here + r, 1), :] * gm_ref[q, j].astype(f32)
        gs_ref[r] = total
        return carry

    lax.fori_loop(0, rows_here, outer, 0, unroll=4)

    @pl.when((p == planes - 1) & (part == pl.num_programs(1) - 1))
    def _():
        for q in range(planes):
            keep(q).wait()


def last_pass(thru, g, table_y, co, gm, held, parts):
    planes, chans, slab, cells = thru.shape
    modes, own = g.shape[2], co.shape[1]
    width = cells // parts
    rows_here = own * chans // (planes * parts)
    field = pl.BlockSpec((1, chans, slab, width), lambda p, h: (p, 0, 0, h))
    whole = pl.BlockSpec(memory_space=pltpu.VMEM)
    shape = jax.ShapeDtypeStruct(thru.shape, bf16)
    return pl.pallas_call(
        last_kernel,
        grid=(planes, parts),
        out_shape=(shape, jax.ShapeDtypeStruct((own * chans, chans, modes), f32), shape),
        in_specs=[
            whole,
            whole,
            pl.BlockSpec((modes, width), lambda p, h: (0, h)),
            whole, whole, whole,
        ],
        out_specs=(
            field,
            pl.BlockSpec((rows_here, chans, modes), lambda p, h: (p * parts + h, 0, 0)),
            pl.BlockSpec(memory_space=pl.ANY),
        ),
        scratch_shapes=[
            pltpu.VMEM((slab // PACK, chans * PACK, modes), bf16),
            pltpu.VMEM((planes * rows_here, modes), f32),
            pltpu.SemaphoreType.DMA((planes,)),
        ],
        compiler_params=pltpu.CompilerParams(vmem_limit_bytes=20 << 20),
        name="last_pass",
    )(thru, g, table_y.T, co, gm, held)


def kernel_shards(nx, ny, flow_field, cotangent, spectral_weight, local_weight, channel_bias):
    planes, chans, slab, cells = flow_field.shape
    across = slab * nx * ny
    own, modes = spectral_weight.shape[0], spectral_weight.shape[3]
    scale_inv = math.sqrt(1.0 / (modes // 2))
    fwd_x = basis_table(across, modes, math.sqrt(2.0 / across))
    fwd_y = basis_table(cells, modes, math.sqrt(2.0 / cells))
    inv_x = basis_table(across, modes, scale_inv)
    inv_y = basis_table(cells, modes, scale_inv)
    out, thru, back, coeffs, grad_mixed = main_pass(
        nx, ny, flow_field, cotangent, spectral_weight, local_weight, channel_bias, fwd_y, inv_y, fwd_x, inv_x)
    grad_field, grad_spectral, out = last_pass(thru, back, fwd_y, coeffs, grad_mixed, out, 2)
    return out, grad_field, grad_spectral.reshape(own, chans, chans, modes)


def solution(mesh):
    nx, ny = mesh.shape["gx"], mesh.shape["gy"]

    def shards(flow_field, cotangent, spectral_weight, local_weight, channel_bias):
        planes, chans, slab, cells = flow_field.shape
        own, modes = spectral_weight.shape[0], spectral_weight.shape[3]
        fits = (
            slab % PACK == 0 and LANES % slab == 0 and modes == LANES
            and nx % 2 == 0 and ny == 4 and (modes // nx) % PACK == 0
            and chans % (2 * LANES // slab) == 0 and chans % PACK == 0
            and cells % (2 * LANES) == 0
            and own * nx * ny == modes and chans % (own * chans // (2 * planes)) == 0
        )
        args = (flow_field, cotangent, spectral_weight, local_weight, channel_bias)
        return kernel_shards(nx, ny, *args) if fits else plain_shards(*args)

    placed = (
        P(None, None, ("gx", "gy"), None),
        P(None, None, ("gx", "gy"), None),
        P(("gx", "gy"), None, None, None),
        P(),
        P(),
    )
    return jax.shard_map(
        shards,
        mesh=mesh,
        in_specs=placed,
        out_specs=(
            P(None, None, ("gx", "gy"), None),
            P(None, None, ("gx", "gy"), None),
            P(("gx", "gy"), None, None, None),
        ),
        check_vma=False,
    )
```
